256 devices in a mesh: pipe: 8 (over x, core), dp: 8 (over z), tensor: 4 (over y).
Axes of the slice: x: 4, y: 4, z: 8, core: 2. Of those that a mesh axis runs over, the one named last changes fastest.
Arguments:
- acts_in: bfloat16 [2, 1024, 4096], P(None, 'dp', 'tensor'), may hold values from -6 to 6
- weights: bfloat16 [8, 4096, 4096], P('pipe', None, 'tensor'), may hold values from -0.046875 to 0.046875
- cotangent: bfloat16 [2, 1024, 4096], P(None, 'dp', 'tensor'), may hold values from -6 to 6
- hist_act: float32 [8, 16], P('pipe'), may hold values from 2 to 12
- hist_weight: float32 [8, 16], P('pipe'), may hold values from 0.01 to 0.1
- hist_grad: float32 [8, 16], P('pipe'), may hold values from 2 to 12
Outputs:
- section_acts: bfloat16 [8, 2, 1024, 4096], P('pipe', None, 'dp', 'tensor')
- section_grads: bfloat16 [8, 2, 1024, 4096], P('pipe', None, 'dp', 'tensor')
- weight_grad: bfloat16 [8, 4096, 4096], P('pipe', 'dp', 'tensor')
- new_hist_act: float32 [8, 16], P('pipe')
- new_hist_weight: float32 [8, 16], P('pipe')
- new_hist_grad: float32 [8, 16], P('pipe')
The draws below stay inside these ranges and needn't reach their ends.
All inputs are finite; a program needn't handle non-finite values.
Results may differ from the reference program's by a relative error of at most 0.025.
Values may be sent and summed in bfloat16 or wider, within the bound.
A program may use at most 128 MiB of HBM per device.

```python
import math
import jax
import jax.numpy as jnp
from jax import lax

D = 4096
ROWS = 128
MICRO = 2
HIST = 16
SECTIONS = 8
BATCH = 1024
N_DP = 8
N_TENSOR = 4


def steps_of(key, dims, split, least, high):
    factor_of, own = 1.0, jax.random.fold_in(key, 6)
    for axis_at, blocks in split:
        draws = jnp.exp(jax.random.uniform(jax.random.fold_in(own, axis_at), (blocks,), jnp.float32, least / len(split), high / len(split)))
        factor_of = factor_of * jnp.repeat(draws, dims[axis_at] // blocks).reshape([-1 if axis == axis_at else 1 for axis in range(len(dims))])
    return factor_of


def centred(rng, shape, scale, reach, pieces=(), kind=jnp.bfloat16):
    factor_of = steps_of(rng, shape, pieces, -0.22, 0.18) if pieces else 1.0
    result = jax.random.normal(rng, shape, jnp.float32) * scale * factor_of
    return jnp.minimum(jnp.maximum(result, -reach), reach).astype(kind)


def setup_inputs(seed: int = 0) -> dict:
    seeds = jax.random.split(jax.random.key(seed), 7)
    acts_in = centred(seeds[0], (MICRO, BATCH, D), 1.0, 6.0, ((1, 8), (2, 4)))
    weights = centred(seeds[1], (SECTIONS, D, D), (4 * D) ** -0.5, 0.046875, ((0, 8), (2, 4)))
    cotangent = centred(seeds[2], (MICRO, BATCH, D), 1.0, 6.0, ((1, 8), (2, 4)))
    hist_act = jnp.clip(jnp.exp(math.log(12.0) - 1.7917595 * jax.random.uniform(seeds[3], (SECTIONS, HIST), jnp.float32) ** steps_of(seeds[3], (SECTIONS, HIST), ((0, 8),), -0.2, 0.2)), 2.0, 12.0)
    hist_weight = jnp.clip(jnp.exp(math.log(0.1) - 2.3025851 * jax.random.uniform(seeds[4], (SECTIONS, HIST), jnp.float32) ** steps_of(seeds[4], (SECTIONS, HIST), ((0, 8),), -0.2, 0.2)), 0.01, 0.1)
    hist_grad = jnp.clip(jnp.exp(math.log(12.0) - 1.7917595 * jax.random.uniform(seeds[5], (SECTIONS, HIST), jnp.float32) ** steps_of(seeds[5], (SECTIONS, HIST), ((0, 8),), -0.2, 0.2)), 2.0, 12.0)
    return {"acts_in": acts_in, "weights": weights, "cotangent": cotangent, "hist_act": hist_act, "hist_weight": hist_weight, "hist_grad": hist_grad}


def quantize(values, factor, limit_value):
    return jnp.clip(values.astype(jnp.float32) * factor, -limit_value, limit_value).astype(jnp.bfloat16)


def settle(values):
    return lax.optimization_barrier(values.astype(jnp.bfloat16)).astype(jnp.float32)


def roll_history(history, newest):
    return jnp.concatenate([newest[:, None], history[:, :-1]], axis=1)


def reference(acts_in, weights, cotangent, hist_act, hist_weight, hist_grad):
    section_count = weights.shape[0]
    full_width = weights.shape[1]
    block_width = full_width // N_TENSOR
    current = acts_in.reshape(-1, full_width)
    act_factors = []
    weight_factors = []
    quant_acts = []
    quant_weights = []
    outputs = []
    act_peaks = []
    weight_peaks = []
    for section_index in range(section_count):
        act_factor = 448.0 / jnp.max(hist_act[section_index])
        weight_factor = 448.0 / jnp.max(hist_weight[section_index])
        quant_weight = quantize(weights[section_index], weight_factor, 448.0)
        quant_act = quantize(current, act_factor, 448.0)
        act_peaks.append(jnp.max(jnp.abs(current.astype(jnp.float32))))
        weight_peaks.append(jnp.max(jnp.abs(weights[section_index].astype(jnp.float32))))
        mixed_terms = jnp.dot(quant_act, quant_weight, preferred_element_type=jnp.float32) * (1.0 / (act_factor * weight_factor))
        current = (current.astype(jnp.float32) + mixed_terms).astype(jnp.bfloat16)
        outputs.append(current.reshape(MICRO, -1, full_width))
        act_factors.append(act_factor)
        weight_factors.append(weight_factor)
        quant_acts.append(quant_act)
        quant_weights.append(quant_weight)
    gradient = (cotangent.reshape(-1, full_width).astype(jnp.float32) * current.astype(jnp.float32)).astype(jnp.bfloat16)
    grads_out = [None] * section_count
    weight_sums = [None] * section_count
    grad_peaks = [None] * section_count
    for section_index in reversed(range(section_count)):
        grad_factor = 57344.0 / jnp.max(hist_grad[section_index])
        grad_peaks[section_index] = jnp.max(jnp.abs(gradient.astype(jnp.float32)))
        quant_grad = quantize(gradient, grad_factor, 57344.0)
        backward_factor = 1.0 / (grad_factor * weight_factors[section_index])
        sum_total = jnp.zeros((gradient.shape[0], full_width), jnp.float32)
        for shard_part in range(N_TENSOR):
            column_span = slice(shard_part * block_width, (shard_part + 1) * block_width)
            product_term = jnp.dot(quant_grad[:, column_span], quant_weights[section_index][:, column_span].T, preferred_element_type=jnp.float32) * backward_factor
            sum_total = sum_total + settle(product_term)
        gradient = (gradient.astype(jnp.float32) + sum_total).astype(jnp.bfloat16)
        grads_out[section_index] = gradient.reshape(MICRO, -1, full_width)
        update_factor = 1.0 / (act_factors[section_index] * grad_factor)
        acts_split = quant_acts[section_index].reshape(MICRO, N_DP, ROWS, full_width)
        grads_split = quant_grad.reshape(MICRO, N_DP, ROWS, full_width)
        weight_sum = jnp.zeros((full_width, full_width), jnp.float32)
        for dp_rank in range(N_DP):
            left_rows = acts_split[:, dp_rank].reshape(-1, full_width)
            right_rows = grads_split[:, dp_rank].reshape(-1, full_width)
            weight_sum = weight_sum + settle(jnp.dot(left_rows.T, right_rows, preferred_element_type=jnp.float32) * update_factor)
        weight_sums[section_index] = weight_sum.astype(jnp.bfloat16)
    section_acts = jnp.stack(outputs)
    section_grads = jnp.stack(grads_out)
    weight_grad = jnp.stack(weight_sums)
    new_hist_act = roll_history(hist_act, jnp.stack(act_peaks))
    new_hist_weight = roll_history(hist_weight, jnp.stack(weight_peaks))
    new_hist_grad = roll_history(hist_grad, jnp.stack(grad_peaks))
    return (section_acts, section_grads, weight_grad, new_hist_act, new_hist_weight, new_hist_grad)
```

```python
import functools

import jax
import jax.numpy as jnp
from jax import lax
from jax.experimental import pallas as pl
from jax.experimental.pallas import tpu as pltpu
from jax.sharding import PartitionSpec as P

MESH = pl.DeviceIdType.MESH
F32 = jnp.float32
BF16 = jnp.bfloat16
CHUNK = 32


def quantize(values, factor, limit):
    return jnp.clip(values.astype(F32) * factor, -limit, limit).astype(BF16)


def gray(j):
    return j ^ (j >> 1)


def kernel(
    S, Z, T, n, R,
    acts, weights, cot, hist_act, hist_weight, hist_grad,
    out_acts, out_grads, out_wgrad, out_peaks,
    w, xg, xq, ar, gr, outv, gin, gout, gq, ps, pr, pr2, rr, cotv, wg, amax, wmax, gmax, pks, pky, pkm, pkz,
    ld_w, ld_x, ld_c, st_o, st_g, st_w,
    f_recv, fg_send, fo_send, a_send, a_recv, p_send, p_recv, p2_send, p2_recv,
    r_send, r_recv, gi_send, gi_recv, go_send, go_recv, z_send, z_recv,
    ky_send, ky_recv, kz_send, kz_recv,
):
    s = lax.axis_index("pipe")
    z = lax.axis_index("dp")
    y = lax.axis_index("tensor")
    H = Z // T
    C = w.shape[1]
    odd = lax.rem(s, 2)
    even = odd == 0
    is_odd = odd == 1
    first = s == 0
    last = s == S - 1
    pair = s + 1 - 2 * odd
    cross = s - 1 + 2 * odd
    has_cross = (cross >= 0) & (cross < S)

    def at_y(d):
        return lax.rem(y + d, T)

    def at_z(d):
        return lax.rem(z + d, Z)

    def rcopy(src, dst, send, recv, **device):
        return pltpu.make_async_remote_copy(
            src_ref=src, dst_ref=dst, send_sem=send, recv_sem=recv, device_id=device, device_id_type=MESH
        )

    barrier = pltpu.get_barrier_semaphore()
    for d in range(1, T):
        pl.semaphore_signal(barrier, inc=1, device_id={"tensor": at_y(d)}, device_id_type=MESH)
    for d in range(1, Z):
        pl.semaphore_signal(barrier, inc=1, device_id={"dp": at_z(d)}, device_id_type=MESH)
    for d in range(T):
        pl.semaphore_signal(barrier, inc=1, device_id={"pipe": pair, "tensor": at_y(d)}, device_id_type=MESH)

    @pl.when(has_cross)
    def _():
        pl.semaphore_signal(barrier, inc=1, device_id={"pipe": cross}, device_id_type=MESH)

    own = pl.ds(y * H, H)

    def load_w(r):
        return pltpu.make_async_copy(weights.at[r], w.at[r], ld_w.at[r])

    def load_x(c, h):
        return pltpu.make_async_copy(
            acts.at[c, :, pl.ds(h * C, C)], xg.at[c, y * H + h], ld_x.at[c, h]
        )

    load_c = pltpu.make_async_copy(cot, cotv, ld_c)

    @pl.when(first)
    def _():
        for h in range(H):
            lax.fori_loop(0, n, lambda c, u: (load_x(c, h).start(), u)[1], 0)

    lax.fori_loop(0, Z, lambda r, u: (load_w(r).start(), u)[1], 0)

    @pl.when(last)
    def _():
        load_c.start()

    ha = jnp.max(hist_act[...], axis=1, keepdims=True)
    hw = jnp.max(hist_weight[...], axis=1, keepdims=True)
    hg = jnp.max(hist_grad[...], axis=1, keepdims=True)
    act_factor = 448.0 / ha
    weight_factor = 448.0 / hw
    grad_factor = 57344.0 / hg
    forward_factor = 1.0 / (act_factor * weight_factor)
    backward_factor = 1.0 / (grad_factor * weight_factor)
    update_factor = 1.0 / (act_factor * grad_factor)

    amax[...] = jnp.zeros_like(amax)
    wmax[...] = jnp.zeros_like(wmax)
    gmax[...] = jnp.zeros_like(gmax)

    @pl.when(first)
    def _():
        for h in range(H):
            lax.fori_loop(0, n, lambda c, u: (load_x(c, h).wait(), u)[1], 0)

    pl.semaphore_wait(barrier, (T - 1) + (Z - 1) + T + has_cross.astype(jnp.int32))

    def fwd_copy(c, k, send, **device):
        return rcopy(xg.at[c, own], xg.at[c, own], send, f_recv.at[c, k], **device)

    def gather_copy(c, d):
        return fwd_copy(c, y, fg_send.at[c, d - 1], tensor=at_y(d))

    def out_copy(c, d):
        return rcopy(
            outv.at[c], xg.at[c, own], fo_send.at[c, d], f_recv.at[c, y], pipe=pair, tensor=at_y(d)
        )

    def hop_copy(c):
        return rcopy(outv.at[c], xg.at[c, own], fo_send.at[c, 0], f_recv.at[c, y], pipe=cross)

    def wait_block(c, yb):
        blk = xg.at[c, pl.ds(yb * H, H)]
        rcopy(blk, blk, fo_send.at[c, 0], f_recv.at[c, yb], pipe=pair).wait_recv()

    def act_copy(c, d):
        r = at_z(d)
        return rcopy(xq.at[c, r], ar.at[c, z], a_send.at[c, d - 1], a_recv.at[c, z], dp=r)

    @pl.when(first)
    def _():
        def go(c, u):
            for d in (2, 1, 3):
                gather_copy(c, d).start()
            return u
        lax.fori_loop(0, n, go, 0)

    def quant_w(r, u):
        load_w(r).wait()
        raw = w[r].astype(F32)
        wmax[...] = jnp.maximum(wmax[...], jnp.max(jnp.abs(raw), axis=0, keepdims=True))
        w[r] = jnp.clip(raw * weight_factor, -448.0, 448.0).astype(BF16)
        return u

    lax.fori_loop(0, Z, quant_w, 0)

    def store_out(c, h):
        return pltpu.make_async_copy(outv.at[c, h], out_acts.at[c, :, pl.ds(h * C, C)], st_o.at[c, h])

    def forward(c, u):
        @pl.when(jnp.logical_not(first))
        def _():
            wait_block(c, y)

            @pl.when(even)
            def _():
                for d in (2, 1, 3):
                    gather_copy(c, d).start()

        total = jnp.zeros((R, H * C), F32)
        for j in range(T):
            yb = at_y(gray(j))
            if j:
                wait_block(c, yb)
            for h in range(H):
                r = yb * H + h
                x = xg[c, r]
                if j == 0:
                    amax[h] = jnp.maximum(amax[h], jnp.max(jnp.abs(x.astype(F32)), axis=0, keepdims=True))
                q = quantize(x, act_factor, 448.0)
                xq[c, r] = q
                total = total + jnp.dot(q, w[r], preferred_element_type=F32)
        for h in range(H):
            o = xg[c, y * H + h].astype(F32) + total[:, h * C : (h + 1) * C] * forward_factor
            outv[c, h] = o.astype(BF16)

        @pl.when(even)
        def _():
            for d in (2, 1, 3, 0):
                out_copy(c, d).start()

        @pl.when(is_odd & has_cross)
        def _():
            hop_copy(c).start()

        for d in range(1, Z):
            act_copy(c, d).start()
        ar[c, z] = xq[c, z]
        for h in range(H):
            store_out(c, h).start()
        return u

    lax.fori_loop(0, n, forward, 0)

    def part_copy(c, d):
        yb = at_y(d)
        return rcopy(ps.at[c, yb], pr.at[c, y], p_send.at[c, d], p_recv.at[c, y], pipe=pair, tensor=yb)

    def peer_copy(c, d):
        yb = at_y(d)
        return rcopy(ps.at[c, yb], pr2.at[c, y], p2_send.at[c, d - 1], p2_recv.at[c, y], tensor=yb)

    def rest_copy(c):
        return rcopy(gin.at[c], rr.at[c], r_send.at[c], r_recv.at[c], pipe=pair)

    def back_copy(c):
        return rcopy(gin.at[c], gout.at[c], go_send.at[c], go_recv.at[c], pipe=pair)

    def g_hop_copy(c):
        return rcopy(gout.at[c], gin.at[c], gi_send.at[c], gi_recv.at[c], pipe=cross)

    def z_copy(c, d):
        return rcopy(gq.at[c], gr.at[c, z], z_send.at[c, d - 1], z_recv.at[c, z], dp=at_z(d))

    def store_g(c):
        return pltpu.make_async_copy(gout.at[c], out_grads.at[c], st_g.at[c])

    @pl.when(last)
    def _():
        load_c.wait()

    def backward(c, u):
        @pl.when(last)
        def _():
            for h in range(H):
                part = cotv[c, :, h * C : (h + 1) * C].astype(F32) * outv[c, h].astype(F32)
                gin[c, :, h * C : (h + 1) * C] = part.astype(BF16)

        @pl.when(even)
        def _():
            rest_copy(c).wait_recv()
            for k in range(T):
                rcopy(pr.at[c, k], pr.at[c, k], p_send.at[c, 0], p_recv.at[c, k], pipe=pair).wait_recv()
            for h in range(H):
                g = rr[c, :, h * C : (h + 1) * C].astype(F32)
                for k in range(T):
                    g = g + pr[c, k, h].astype(F32)
                gin[c, :, h * C : (h + 1) * C] = g.astype(BF16)
            back_copy(c).start()

        @pl.when(is_odd & has_cross)
        def _():
            g_hop_copy(c).wait_recv()

        g = gin[c]
        gmax[...] = jnp.maximum(gmax[...], jnp.max(jnp.abs(g.astype(F32)), axis=0, keepdims=True))
        q = quantize(g, grad_factor, 57344.0)
        gq[c] = q

        @pl.when(is_odd)
        def _():
            rest_copy(c).start()

        for d in (2, 1, 3, 0):
            yb = at_y(d)
            for h in range(H):
                part = lax.dot_general(
                    q, w[yb * H + h], (((1,), (1,)), ((), ())), preferred_element_type=F32
                )
                ps[c, yb, h] = (part * backward_factor).astype(BF16)

            @pl.when(is_odd)
            def _():
                part_copy(c, d).start()

            if d:
                @pl.when(even)
                def _():
                    peer_copy(c, d).start()

        for d in range(1, Z):
            z_copy(c, d).start()
        gr[c, z] = q

        @pl.when(even)
        def _():
            for d in (3, 1, 2):
                k = at_y(d)
                rcopy(pr2.at[c, k], pr2.at[c, k], p_send.at[c, 0], p2_recv.at[c, k], pipe=pair).wait_recv()
            for h in range(H):
                g = gin[c, :, h * C : (h + 1) * C].astype(F32)
                g = g + ps[c, y, h].astype(F32)
                for d in range(1, T):
                    g = g + pr2[c, at_y(d), h].astype(F32)
                gout[c, :, h * C : (h + 1) * C] = g.astype(BF16)

            @pl.when(has_cross)
            def _():
                g_hop_copy(c).start()
            store_g(c).start()

        return u

    lax.fori_loop(0, n, backward, 0)

    lanes = pks.shape[-1]
    peak_a = jnp.max(jnp.maximum(amax[0], amax[H - 1]), axis=1, keepdims=True)
    peak_w = jnp.max(wmax[...], axis=1, keepdims=True)
    peak_g = jnp.max(gmax[...], axis=1, keepdims=True)
    row = lax.broadcasted_iota(jnp.int32, (8, lanes), 0)
    tile = jnp.where(row == 0, peak_a, jnp.where(row == 1, peak_w, peak_g))
    pks[...] = tile

    def ky_copy(d):
        return rcopy(pks, pky.at[y], ky_send.at[d - 1], ky_recv.at[y], tensor=at_y(d))

    def kz_copy(d):
        return rcopy(pkm, pkz.at[z], kz_send.at[d - 1], kz_recv.at[z], dp=at_z(d))

    for d in range(1, T):
        ky_copy(d).start()
    for d in range(1, T):
        k = at_y(d)
        rcopy(pks, pky.at[k], ky_send.at[0], ky_recv.at[k], tensor=k).wait_recv()
        tile = jnp.maximum(tile, pky[k])
    pkm[...] = tile
    for d in range(1, Z):
        kz_copy(d).start()

    def wait_rows(c, u):
        for d in range(1, Z):
            k = at_z(d)
            rcopy(ar.at[c, k], ar.at[c, k], z_send.at[c, 0], a_recv.at[c, k], dp=k).wait_recv()
            rcopy(gr.at[c, k], gr.at[c, k], z_send.at[c, 0], z_recv.at[c, k], dp=k).wait_recv()
        return u

    lax.fori_loop(0, n, wait_rows, 0)
    left = ar[...].reshape(n * Z * R, C)
    right = gr[...].reshape(n * Z * R, H * C)
    prod = lax.dot_general(left, right, (((0,), (0,)), ((), ())), preferred_element_type=F32)
    wg[...] = (prod * update_factor).astype(BF16)
    st = pltpu.make_async_copy(wg, out_wgrad, st_w)
    st.start()

    for d in range(1, Z):
        k = at_z(d)
        rcopy(pkm, pkz.at[k], kz_send.at[0], kz_recv.at[k], dp=k).wait_recv()
        tile = jnp.maximum(tile, pkz[k])
    out_peaks[...] = tile

    for d in range(1, T):
        ky_copy(d).wait_send()
    for d in range(1, Z):
        kz_copy(d).wait_send()

    def close(c, u):
        @pl.when(even)
        def _():
            for d in range(1, T):
                gather_copy(c, d).wait_send()
                peer_copy(c, d).wait_send()
            for d in range(T):
                out_copy(c, d).wait_send()
            back_copy(c).wait_send()

            @pl.when(has_cross)
            def _():
                g_hop_copy(c).wait_send()

        @pl.when(is_odd)
        def _():
            for d in range(T):
                part_copy(c, d).wait_send()
            rest_copy(c).wait_send()
            back_copy(c).wait_recv()
            store_g(c).start()

            @pl.when(has_cross)
            def _():
                hop_copy(c).wait_send()

        for d in range(1, Z):
            act_copy(c, d).wait_send()
            z_copy(c, d).wait_send()
        for h in range(H):
            store_out(c, h).wait()
        return u

    lax.fori_loop(0, n, close, 0)
    lax.fori_loop(0, n, lambda c, u: (store_g(c).wait(), u)[1], 0)
    st.wait()


def step(acts_in, weights, cotangent, hist_act, hist_weight, hist_grad):
    S, Z, T = (lax.axis_size(a) for a in ("pipe", "dp", "tensor"))
    micro, rows, width = acts_in.shape
    depth = weights.shape[1]
    R = min(CHUNK, rows)
    n = micro * rows // R
    H = Z // T
    C = depth // Z
    acts = acts_in.reshape(n, R, width)
    cot = cotangent.reshape(n, R, width)
    w = weights.reshape(Z, C, width)
    any_ = pl.BlockSpec(memory_space=pl.ANY)
    vmem = pl.BlockSpec(memory_space=pltpu.VMEM)
    dma = pltpu.SemaphoreType.DMA
    b = lambda *shape: pltpu.VMEM(shape, BF16)
    f = lambda *shape: pltpu.VMEM(shape, F32)
    out_acts, out_grads, out_w, peaks = pl.pallas_call(
        functools.partial(kernel, S, Z, T, n, R),
        out_shape=(
            jax.ShapeDtypeStruct((n, R, width), BF16),
            jax.ShapeDtypeStruct((n, R, width), BF16),
            jax.ShapeDtypeStruct((C, width), BF16),
            jax.ShapeDtypeStruct((8, 128), F32),
        ),
        in_specs=[any_, any_, any_, vmem, vmem, vmem],
        out_specs=(any_, any_, any_, vmem),
        scratch_shapes=[
            b(Z, C, width), b(n, Z, R, C), b(n, Z, R, C), b(n, Z, R, C), b(n, Z, R, width),
            b(n, H, R, C), b(n, R, width), b(n, R, width), b(n, R, width),
            b(n, T, H, R, C), b(n, T, H, R, C), b(n, T, H, R, C), b(n, R, width), b(n, R, width),
            b(C, width), f(H, 1, C), f(1, width), f(1, width),
            f(8, 128), f(T, 8, 128), f(8, 128), f(Z, 8, 128),
            dma((Z,)), dma((n, H)), dma, dma((n, H)), dma((n,)), dma,
            dma((n, T)), dma((n, T - 1)), dma((n, T)), dma((n, Z - 1)), dma((n, Z)),
            dma((n, T)), dma((n, T)), dma((n, T - 1)), dma((n, T)),
            dma((n,)), dma((n,)), dma((n,)), dma((n,)), dma((n,)), dma((n,)),
            dma((n, Z - 1)), dma((n, Z)),
            dma((T - 1,)), dma((T,)), dma((Z - 1,)), dma((Z,)),
        ],
        compiler_params=pltpu.CompilerParams(
            collective_id=0, has_side_effects=True, vmem_limit_bytes=60 * 1024 * 1024
        ),
    )(acts, w, cot, hist_act, hist_weight, hist_grad)

    def roll(history, newest):
        return jnp.concatenate([newest, history[:, :-1]], axis=1)

    return (
        out_acts.reshape(1, micro, rows, width),
        out_grads.reshape(1, micro, rows, width),
        out_w[None],
        roll(hist_act, peaks[0:1, 0:1]),
        roll(hist_weight, peaks[1:2, 0:1]),
        roll(hist_grad, peaks[2:3, 0:1]),
    )


def solution(mesh):
    placed = (
        P(None, "dp", "tensor"),
        P("pipe", None, "tensor"),
        P(None, "dp", "tensor"),
        P("pipe", None),
        P("pipe", None),
        P("pipe", None),
    )
    return jax.shard_map(
        step,
        mesh=mesh,
        in_specs=placed,
        out_specs=(
            P("pipe", None, "dp", "tensor"),
            P("pipe", None, "dp", "tensor"),
            P("pipe", "dp", "tensor"),
            P("pipe", None),
            P("pipe", None),
            P("pipe", None),
        ),
        check_vma=False,
    )
```

```python
import contextlib
import functools

import jax
import jax.numpy as jnp
from jax import lax
from jax.experimental import pallas as pl
from jax.experimental.pallas import tpu as pltpu
from jax.sharding import PartitionSpec as P

MESH = pl.DeviceIdType.MESH
F32 = jnp.float32
BF16 = jnp.bfloat16
CHUNK = 16
AHEAD = 3
LAG = 4

scope = lambda name: contextlib.nullcontext()


def quantize(values, factor, limit):
    return jnp.clip(values.astype(F32) * factor, -limit, limit).astype(BF16)


def gray(j):
    return j ^ (j >> 1)


def kernel(
    S, Z, T, n, R,
    acts, weights, cot, hist_act, hist_weight, hist_grad,
    out_acts, out_grads, out_wgrad, out_peaks,
    w, wt, xg, xq, ar, gr, outv, gin, gout, gq, ps, pr, pr0, cotv, acc, wg, amax, wmax, gmax, pks, pky, pkm, pkz,
    ld_w, ld_x, ld_c, st_o, st_g, st_w,
    f_recv, fg_send, fo_send, a_send, a_recv, p_send, p_recv, p0_recv, go_send, go_recv, z_send, zf_recv, zo_recv,
    ky_send, ky_recv, kz_send, kz_recv,
):
    s = lax.axis_index("pipe")
    z = lax.axis_index("dp")
    y = lax.axis_index("tensor")
    H = Z // T
    C = w.shape[1]
    odd = lax.rem(s, 2)
    even = odd == 0
    is_odd = odd == 1
    first = s == 0
    last = s == S - 1
    not_last = jnp.logical_not(last)
    not_first = jnp.logical_not(first)
    up = jnp.minimum(s + 1, S - 1)
    down = jnp.maximum(s - 1, 0)

    def at_y(d):
        return lax.rem(y + d, T)

    def at_z(d):
        return lax.rem(z + d, Z)

    def rcopy(src, dst, send, recv, **device):
        return pltpu.make_async_remote_copy(
            src_ref=src, dst_ref=dst, send_sem=send, recv_sem=recv, device_id=device, device_id_type=MESH
        )

    def drain_send(sem, ref):
        rcopy(ref, ref, sem, sem, tensor=at_y(1)).wait_send()

    def drain_recv(sem, ref):
        rcopy(ref, ref, sem, sem, tensor=at_y(1)).wait_recv()

    barrier = pltpu.get_barrier_semaphore()
    for d in range(1, T):
        pl.semaphore_signal(barrier, inc=1, device_id={"tensor": at_y(d)}, device_id_type=MESH)
    for d in range(1, Z):
        pl.semaphore_signal(barrier, inc=1, device_id={"dp": at_z(d)}, device_id_type=MESH)
    for d in range(T):
        @pl.when(not_last)
        def _():
            pl.semaphore_signal(barrier, inc=1, device_id={"pipe": up, "tensor": at_y(d)}, device_id_type=MESH)

        @pl.when(not_first)
        def _():
            pl.semaphore_signal(barrier, inc=1, device_id={"pipe": down, "tensor": at_y(d)}, device_id_type=MESH)

    own = pl.ds(y * H, H)

    def load_w(r):
        return pltpu.make_async_copy(weights.at[r], w.at[r], ld_w.at[r])

    def load_x(c, h):
        return pltpu.make_async_copy(
            acts.at[c, :, pl.ds(h * C, C)], xg.at[c, y * H + h], ld_x
        )

    load_c = pltpu.make_async_copy(cot, cotv, ld_c)

    @pl.when(first)
    def _():
        for h in range(H):
            lax.fori_loop(0, n, lambda c, u: (load_x(c, h).start(), u)[1], 0)

    lax.fori_loop(0, Z, lambda r, u: (load_w(r).start(), u)[1], 0)

    @pl.when(last)
    def _():
        load_c.start()

    ha = jnp.max(hist_act[...], axis=1, keepdims=True)
    hw = jnp.max(hist_weight[...], axis=1, keepdims=True)
    hg = jnp.max(hist_grad[...], axis=1, keepdims=True)
    act_factor = 448.0 / ha
    weight_factor = 448.0 / hw
    grad_factor = 57344.0 / hg
    forward_factor = 1.0 / (act_factor * weight_factor)
    backward_factor = 1.0 / (grad_factor * weight_factor)
    update_factor = 1.0 / (act_factor * grad_factor)

    amax[...] = jnp.zeros_like(amax)
    wmax[...] = jnp.zeros_like(wmax)
    gmax[...] = jnp.zeros_like(gmax)

    @pl.when(first)
    def _():
        pltpu.make_async_copy(xg.at[:, own], xg.at[:, own], ld_x).wait()


    def gather_copy(c, d):
        return rcopy(xg.at[c, own], xg.at[c, own], fg_send, f_recv.at[c, y], tensor=at_y(d))

    def out_copy(c, d):
        return rcopy(outv.at[c], xg.at[c, own], fo_send, f_recv.at[c, y], pipe=up, tensor=at_y(d))

    def wait_block(c, yb):
        drain_recv(f_recv.at[c, yb], xg.at[c, pl.ds(yb * H, H)])

    def act_copy(c, d):
        r = at_z(d)
        return rcopy(xq.at[c, r], ar.at[c, z], a_send, a_recv.at[(c == n - 1).astype(jnp.int32)], dp=r)

    def quant_w(r, u):
        load_w(r).wait()
        raw = w[r].astype(F32)
        wmax[...] = jnp.maximum(wmax[...], jnp.max(jnp.abs(raw), axis=0, keepdims=True))
        w[r] = jnp.clip(raw * weight_factor, -448.0, 448.0).astype(BF16)
        return u

    def turn_w(r, u):
        wt[r] = w[r].T
        return u

    with scope("qw"):
        lax.fori_loop(0, Z, quant_w, 0)

    with scope("barrier"):
        pairs = not_first.astype(jnp.int32) + not_last.astype(jnp.int32)
        pl.semaphore_wait(barrier, (T - 1) + (Z - 1) + T * pairs)

    def start_gather(c):
        for d in (2, 1, 3):
            gather_copy(c, d).start()

    @pl.when(first)
    def _():
        for c in range(AHEAD):
            start_gather(c)

    late = s >= S // 2
    early = jnp.logical_not(late)

    @pl.when(late)
    def _():
        with scope("turn"):
            lax.fori_loop(0, Z, turn_w, 0)

    def store_out(c, h):
        return pltpu.make_async_copy(outv.at[c, h], out_acts.at[c, :, pl.ds(h * C, C)], st_o)

    def forward(c):
        @pl.when(first & (c + AHEAD < n))
        def _():
            start_gather(c + AHEAD)

        total = jnp.zeros((R, H * C), F32)
        for j in range(T):
            yb = at_y((2 * (1 - odd), 1, 3, 2 * odd)[j])

            if j < T - 1:
                with scope(f"fwait{j}"):
                    wait_block(c, yb)
            else:
                @pl.when(not_first)
                def _():
                    with scope(f"fwait{j}"):
                        wait_block(c, yb)

            for h in range(H):
                r = yb * H + h
                x = xg[c, r]
                q = quantize(x, act_factor, 448.0)
                xq[c, r] = q
                total = total + jnp.dot(q, w[r], preferred_element_type=F32)
        for h in range(H):
            x = xg[c, y * H + h].astype(F32)
            outv[c, h] = (x + total[:, h * C : (h + 1) * C] * forward_factor).astype(BF16)

        @pl.when(not_last)
        def _():
            for d in (2, 1, 3, 0):
                out_copy(c, d).start()

        with scope("fz"):
            for d in (4, 3, 5, 2, 6, 1, 7):
                act_copy(c, d).start()
            ar[c, z] = xq[c, z]
            for h in range(H):
                store_out(c, h).start()
                x = xg[c, y * H + h].astype(F32)
                amax[h] = jnp.maximum(amax[h], jnp.max(jnp.abs(x), axis=0, keepdims=True))

    def part_copy(c, d):
        yb = at_y(d)
        return rcopy(ps.at[c, yb], pr.at[c, y], p_send, p_recv.at[c], pipe=down, tensor=yb)

    def peer_copy(c, d):
        yb = at_y(d)
        return rcopy(ps.at[c, yb], pr0.at[c, y], p_send, p0_recv, tensor=yb)

    def back_copy(c):
        return rcopy(gin.at[c], gout.at[c], go_send, go_recv, pipe=up)

    def z_copy(c, d):
        if d == 2:
            recv = zf_recv.at[c, 0]
        elif d == Z - 2:
            recv = zf_recv.at[c, 1]
        else:
            recv = zo_recv.at[(c == n - 1).astype(jnp.int32)]
        return rcopy(gq.at[c], gr.at[c, z], z_send, recv, dp=at_z(d))

    def relay_copies(c):
        lo, hi = at_z(Z - 2), at_z(2)
        half = H * C // 2
        out = []
        for k, dest, part in (
            (lo, 1, pl.ds(0, 2 * half)), (hi, Z - 1, pl.ds(0, 2 * half)),
            (lo, 2, pl.ds(0, half)), (hi, Z - 2, pl.ds(half, half)),
        ):
            ref = gr.at[c, k, :, part]
            out.append(rcopy(ref, ref, z_send, zo_recv.at[0], dp=at_z(dest)))
        return out

    def wait_far(c):
        drain_recv(zf_recv.at[c, 0], gr.at[c, at_z(Z - 2)])
        drain_recv(zf_recv.at[c, 1], gr.at[c, at_z(2)])

    def relay(c):
        with scope("relay"):
            wait_far(c)
            for r in relay_copies(c):
                r.start()

    def store_g(c):
        return pltpu.make_async_copy(gout.at[c], out_grads.at[c], st_g)

    @pl.when(last)
    def _():
        load_c.wait()

    def backward(c):
        @pl.when(last)
        def _():
            for h in range(H):
                part = cotv[c, :, h * C : (h + 1) * C].astype(F32) * outv[c, h].astype(F32)
                gin[c, :, h * C : (h + 1) * C] = part.astype(BF16)

        @pl.when(not_last)
        def _():
            with scope("bwait"):
                drain_recv(p_recv.at[c], pr.at[c])
            for h in range(H):
                g = pr[c, 0, h].astype(F32)
                for k in range(1, T):
                    g = g + pr[c, k, h].astype(F32)
                gin[c, :, h * C : (h + 1) * C] = g.astype(BF16)

        g = gin[c]
        q = quantize(g, grad_factor, 57344.0)
        gq[c] = q

        for d in (2, 1, 3, 0):
            yb = at_y(d)
            for h in range(H):
                part = jnp.dot(q, wt[yb * H + h], preferred_element_type=F32) * backward_factor
                if d == 0:
                    part = part + g[:, h * C : (h + 1) * C].astype(F32)
                ps[c, yb, h] = part.astype(BF16)

            @pl.when(not_first)
            def _():
                part_copy(c, d).start()

            if d:
                @pl.when(first)
                def _():
                    peer_copy(c, d).start()

        with scope("bz"):
            for d in (2, Z - 2, 1, Z - 1):
                z_copy(c, d).start()

            @pl.when(c == n - 1)
            def _():
                for d in range(3, Z - 2):
                    z_copy(c, d).start()

            @pl.when(not_last)
            def _():
                back_copy(c).start()

            gmax[...] = jnp.maximum(gmax[...], jnp.max(jnp.abs(g.astype(F32)), axis=0, keepdims=True))
            gr[c, z] = q

        @pl.when((c >= LAG) & early)
        def _():
            relay(c - LAG)

    def slot(k, u):
        ahead = jnp.where(last, lax.rem(k, 2) == 0, k < n)
        c = jnp.where(last, k // 2, lax.rem(k, n))

        @pl.when(ahead)
        def _():
            forward(c)

        @pl.when(jnp.logical_not(ahead))
        def _():
            backward(c)

        @pl.when(early & (k == n - 1))
        def _():
            with scope("turn"):
                lax.fori_loop(0, Z, turn_w, 0)

        return u

    lax.fori_loop(0, 2 * n, slot, 0)
    lax.fori_loop(jnp.where(early, n - LAG, 0), n - 1, lambda c, u: (relay(c), u)[1], 0)

    lanes = pks.shape[-1]
    peak_a = jnp.max(jnp.maximum(amax[0], amax[H - 1]), axis=1, keepdims=True)
    peak_w = jnp.max(wmax[...], axis=1, keepdims=True)
    peak_g = jnp.max(gmax[...], axis=1, keepdims=True)
    row = lax.broadcasted_iota(jnp.int32, (8, lanes), 0)
    tile = jnp.where(row == 0, peak_a, jnp.where(row == 1, peak_w, peak_g))
    pks[...] = tile

    def ky_copy(d):
        return rcopy(pks, pky.at[y], ky_send, ky_recv, tensor=at_y(d))

    def kz_copy(d):
        return rcopy(pkm, pkz.at[z], kz_send, kz_recv, dp=at_z(d))

    for d in range(1, T):
        ky_copy(d).start()
    with scope("kwait"):
        drain_recv(ky_recv, pky.at[pl.ds(0, T - 1)])
    pky[y] = tile
    for k in range(T):
        tile = jnp.maximum(tile, pky[k])
    pkm[...] = tile
    for d in range(1, Z):
        kz_copy(d).start()

    @pl.when(first)
    def _():
        def finish(c, u):
            for h in range(H):
                g = ps[c, y, h].astype(F32)
                for d in range(1, T):
                    g = g + pr0[c, at_y(d), h].astype(F32)
                gout[c, :, h * C : (h + 1) * C] = g.astype(BF16)
            return u

        with scope("first"):
            drain_recv(p0_recv, pr0.at[:, pl.ds(0, T - 1)])
            lax.fori_loop(0, n, finish, 0)

    @pl.when(not_first)
    def _():
        with scope("backwait"):
            drain_recv(go_recv, gout)

    lax.fori_loop(0, n, lambda c, u: (store_g(c).start(), u)[1], 0)

    def rows_product(lo, count):
        left = ar[lo : lo + count].reshape(count * Z * R, C)
        right = gr[lo : lo + count].reshape(count * Z * R, H * C)
        return lax.dot_general(left, right, (((0,), (0,)), ((), ())), preferred_element_type=F32)

    with scope("zwait"):
        drain_recv(a_recv.at[0], ar.at[pl.ds(0, n - 1), pl.ds(0, Z - 1)])
        drain_recv(zo_recv.at[0], gr.at[pl.ds(0, n - 1), pl.ds(0, Z - 3)])
    with scope("wgrad"):
        acc[...] = rows_product(0, n - 1)
    with scope("zwait_last"):
        drain_recv(a_recv.at[1], ar.at[n - 1, pl.ds(0, Z - 1)])
        drain_recv(zo_recv.at[1], gr.at[n - 1, pl.ds(0, Z - 3)])
        wait_far(n - 1)
    with scope("wgrad_last"):
        wg[...] = ((acc[...] + rows_product(n - 1, 1)) * update_factor).astype(BF16)
    st = pltpu.make_async_copy(wg, out_wgrad, st_w)
    st.start()

    drain_recv(kz_recv, pkz.at[pl.ds(0, Z - 1)])
    pkz[z] = tile
    for k in range(Z):
        tile = jnp.maximum(tile, pkz[k])
    out_peaks[...] = tile

    with scope("close"):
        drain_send(ky_send, pky.at[pl.ds(0, T - 1)])
        drain_send(kz_send, pkz.at[pl.ds(0, Z - 1)])
        drain_send(a_send, ar.at[:, pl.ds(0, Z - 1)])
        drain_send(z_send, gr.at[:, pl.ds(0, Z - 1)])

        @pl.when(first)
        def _():
            drain_send(fg_send, pr.at[:, pl.ds(0, T - 1)])
            drain_send(p_send, pr.at[:, pl.ds(0, T - 1)])

        @pl.when(not_first)
        def _():
            drain_send(p_send, pr)

        @pl.when(not_last)
        def _():
            drain_send(fo_send, pr)
            drain_send(go_send, gin)

        pltpu.make_async_copy(outv, outv, st_o).wait()
        pltpu.make_async_copy(gout, gout, st_g).wait()
        st.wait()


def finish_kernel(a, g, m, peaks, ha, hw, hg, oa, og, om, na, nw, ng, va, vg, vm, load, store):
    loads = [pltpu.make_async_copy(x, v, load.at[i]) for i, (x, v) in enumerate(((a, va), (g, vg), (m, vm)))]
    stores = [pltpu.make_async_copy(v, o, store.at[i]) for i, (v, o) in enumerate(((va, oa), (vg, og), (vm, om)))]
    for c in loads:
        c.start()
    for i, (old, new) in enumerate(((ha, na), (hw, nw), (hg, ng))):
        new[:, 1:] = old[:, :-1]
        new[:, 0:1] = peaks[i : i + 1, 0:1]
    for c, d in zip(loads, stores):
        c.wait()
        d.start()
    for d in stores:
        d.wait()


def step(acts_in, weights, cotangent, hist_act, hist_weight, hist_grad):
    S, Z, T = (lax.axis_size(a) for a in ("pipe", "dp", "tensor"))
    micro, rows, width = acts_in.shape
    depth = weights.shape[1]
    R = min(CHUNK, rows)
    n = micro * rows // R
    H = Z // T
    C = depth // Z
    acts = acts_in.reshape(n, R, width)
    cot = cotangent.reshape(n, R, width)
    w = weights.reshape(Z, C, width)
    any_ = pl.BlockSpec(memory_space=pl.ANY)
    hbm = pl.BlockSpec(memory_space=pltpu.HBM)
    vmem = pl.BlockSpec(memory_space=pltpu.VMEM)
    dma = pltpu.SemaphoreType.DMA
    b = lambda *shape: pltpu.VMEM(shape, BF16)
    f = lambda *shape: pltpu.VMEM(shape, F32)
    out_acts, out_grads, out_w, peaks = pl.pallas_call(
        functools.partial(kernel, S, Z, T, n, R),
        out_shape=(
            jax.ShapeDtypeStruct((n, R, width), BF16),
            jax.ShapeDtypeStruct((n, R, width), BF16),
            jax.ShapeDtypeStruct((C, width), BF16),
            jax.ShapeDtypeStruct((8, 128), F32),
        ),
        in_specs=[any_, any_, any_, vmem, vmem, vmem],
        out_specs=(any_, any_, any_, vmem),
        scratch_shapes=[
            b(Z, C, width), b(Z, width, C), b(n, Z, R, C), b(n, Z, R, C), b(n, Z, R, C), b(n, Z, R, width),
            b(n, H, R, C), b(n, R, width), b(n, R, width), b(n, R, width),
            b(n, T, H, R, C), b(n, T, H, R, C), b(n, T, H, R, C), b(n, R, width), f(C, width),
            b(C, width), f(H, 1, C), f(1, width), f(1, width),
            f(8, 128), f(T, 8, 128), f(8, 128), f(Z, 8, 128),
            dma((Z,)), *(dma,) * 5,
            dma((n, T)), dma, dma, dma, dma((2,)), dma, dma((n,)), dma, dma, dma, dma, dma((n, 2)), dma((2,)),
            *(dma,) * 4,
        ],
        compiler_params=pltpu.CompilerParams(
            collective_id=0, has_side_effects=True, vmem_limit_bytes=60 * 1024 * 1024
        ),
    )(acts, w, cot, hist_act, hist_weight, hist_grad)

    final = pl.pallas_call(
        finish_kernel,
        out_shape=(
            jax.ShapeDtypeStruct((n, R, width), BF16),
            jax.ShapeDtypeStruct((n, R, width), BF16),
            jax.ShapeDtypeStruct((C, width), BF16),
            *(jax.ShapeDtypeStruct(hist_act.shape, F32) for _ in range(3)),
        ),
        in_specs=[hbm, hbm, hbm, vmem, vmem, vmem, vmem],
        out_specs=(hbm, hbm, hbm, vmem, vmem, vmem),
        scratch_shapes=[b(n, R, width), b(n, R, width), b(C, width), dma((3,)), dma((3,))],
        compiler_params=pltpu.CompilerParams(vmem_limit_bytes=8 * 1024 * 1024),
    )(out_acts, out_grads, out_w, peaks, hist_act, hist_weight, hist_grad)
    return (
        final[0].reshape(1, micro, rows, width),
        final[1].reshape(1, micro, rows, width),
        final[2][None],
        *final[3:],
    )


def solution(mesh):
    placed = (
        P(None, "dp", "tensor"),
        P("pipe", None, "tensor"),
        P(None, "dp", "tensor"),
        P("pipe", None),
        P("pipe", None),
        P("pipe", None),
    )
    return jax.shard_map(
        step,
        mesh=mesh,
        in_specs=placed,
        out_specs=(
            P("pipe", None, "dp", "tensor"),
            P("pipe", None, "dp", "tensor"),
            P("pipe", "dp", "tensor"),
            P("pipe", None),
            P("pipe", None),
            P("pipe", None),
        ),
        check_vma=False,
    )
```

```python
import contextlib
import functools

import jax
import jax.numpy as jnp
from jax import lax
from jax.experimental import pallas as pl
from jax.experimental.pallas import tpu as pltpu
from jax.sharding import PartitionSpec as P

MESH = pl.DeviceIdType.MESH
F32 = jnp.float32
BF16 = jnp.bfloat16
CHUNK = 16
AHEAD = 5
WARM = 8

scope = lambda name: contextlib.nullcontext()


def quantize(values, factor, limit):
    return jnp.clip(values.astype(F32) * factor, -limit, limit).astype(BF16)


def gray(j):
    return j ^ (j >> 1)


def kernel(
    S, Z, T, n, R,
    acts, weights, cot, hist_act, hist_weight, hist_grad,
    out_acts, out_grads, out_wgrad, out_peaks,
    w, wt, xg, xq, ar, gr, outv, gin, gout, gq, ps, pr, cotv, acc, wg, amax, wmax, gmax, pks, pky, pkm, pkz,
    ld_w, ld_x, ld_c, st_o, st_g, st_w,
    f_recv, fg_send, fo_send, a_send, a_recv, ay_send, ay_recv, p_send, p_recv, go_send, go_recv,
    z_send, zr_recv, zo_recv,
    ky_send, ky_recv, kz_send, kz_recv,
):
    s = lax.axis_index("pipe")
    z = lax.axis_index("dp")
    y = lax.axis_index("tensor")
    H = Z // T
    C = w.shape[1]
    U = n // 2
    Q = n // T
    odd = lax.rem(s, 2)
    even = odd == 0
    is_odd = odd == 1
    first = s == 0
    last = s == S - 1
    not_last = jnp.logical_not(last)
    not_first = jnp.logical_not(first)
    up = jnp.minimum(s + 1, S - 1)
    down = jnp.maximum(s - 1, 0)

    def at_y(d):
        return lax.rem(y + d, T)

    def at_z(d):
        return lax.rem(z + d, Z)

    def rcopy(src, dst, send, recv, **device):
        return pltpu.make_async_remote_copy(
            src_ref=src, dst_ref=dst, send_sem=send, recv_sem=recv, device_id=device, device_id_type=MESH
        )

    def drain_send(sem, ref):
        rcopy(ref, ref, sem, sem, tensor=at_y(1)).wait_send()

    def drain_recv(sem, ref):
        rcopy(ref, ref, sem, sem, tensor=at_y(1)).wait_recv()

    barrier = pltpu.get_barrier_semaphore()
    for d in range(1, T):
        pl.semaphore_signal(barrier, inc=1, device_id={"tensor": at_y(d)}, device_id_type=MESH)
    for d in range(1, Z):
        pl.semaphore_signal(barrier, inc=1, device_id={"dp": at_z(d)}, device_id_type=MESH)
    for d in range(T):
        @pl.when(not_last)
        def _():
            pl.semaphore_signal(barrier, inc=1, device_id={"pipe": up, "tensor": at_y(d)}, device_id_type=MESH)

        @pl.when(not_first)
        def _():
            pl.semaphore_signal(barrier, inc=1, device_id={"pipe": down, "tensor": at_y(d)}, device_id_type=MESH)

    own = pl.ds(y * H, H)

    def load_w(r):
        return pltpu.make_async_copy(weights.at[r], w.at[r], ld_w.at[r])

    def load_x(c, h):
        return pltpu.make_async_copy(
            acts.at[c, :, pl.ds(h * C, C)], xg.at[c, y * H + h], ld_x
        )

    load_c = pltpu.make_async_copy(cot, cotv, ld_c)

    @pl.when(first)
    def _():
        for h in range(H):
            lax.fori_loop(0, n, lambda c, u: (load_x(c, h).start(), u)[1], 0)

    lax.fori_loop(0, Z, lambda r, u: (load_w(r).start(), u)[1], 0)

    @pl.when(last)
    def _():
        load_c.start()

    ha = jnp.max(hist_act[...], axis=1, keepdims=True)
    hw = jnp.max(hist_weight[...], axis=1, keepdims=True)
    hg = jnp.max(hist_grad[...], axis=1, keepdims=True)
    act_factor = 448.0 / ha
    weight_factor = 448.0 / hw
    grad_factor = 57344.0 / hg
    forward_factor = 1.0 / (act_factor * weight_factor)
    backward_factor = 1.0 / (grad_factor * weight_factor)
    update_factor = 1.0 / (act_factor * grad_factor)

    amax[...] = jnp.zeros_like(amax)
    wmax[...] = jnp.zeros_like(wmax)
    gmax[...] = jnp.zeros_like(gmax)

    @pl.when(first)
    def _():
        pltpu.make_async_copy(xg.at[:, own], xg.at[:, own], ld_x).wait()


    def gather_copy(c, d):
        return rcopy(xg.at[c, own], xg.at[c, own], fg_send, f_recv.at[c, y], tensor=at_y(d))

    def out_copy(c, d):
        return rcopy(outv.at[c], xg.at[c, own], fo_send, f_recv.at[c, y], pipe=up, tensor=at_y(d))

    def wait_block(c, yb):
        drain_recv(f_recv.at[c, yb], xg.at[c, pl.ds(yb * H, H)])

    def act_copy(c, m, d):
        r = at_z(d)
        span = pl.ds(c, m)
        return rcopy(xq.at[span, r], ar.at[span, z], a_send, a_recv, dp=r)

    def share_copy(d):
        span = pl.ds(y * Q, Q)
        return rcopy(ar.at[span], ar.at[span], ay_send, ay_recv, tensor=at_y(d))

    def share_acts():
        with scope("share"):
            drain_recv(a_recv, ar.at[pl.ds(0, Q), pl.ds(0, Z - 1)])
            for d in (2, 1, 3):
                share_copy(d).start()

    def quant_w(r, u):
        load_w(r).wait()
        raw = w[r].astype(F32)
        wmax[...] = jnp.maximum(wmax[...], jnp.max(jnp.abs(raw), axis=0, keepdims=True))
        w[r] = jnp.clip(raw * weight_factor, -448.0, 448.0).astype(BF16)
        return u

    def turn_w(k, u):
        for h in range(H):
            wt[k, :, h * C : (h + 1) * C] = w[k * H + h].T
        return u

    with scope("qw"):
        lax.fori_loop(0, Z, quant_w, 0)

    with scope("barrier"):
        pairs = not_first.astype(jnp.int32) + not_last.astype(jnp.int32)
        pl.semaphore_wait(barrier, (T - 1) + (Z - 1) + T * pairs)

    def start_gather(c):
        for d in (2, 1, 3):
            gather_copy(c, d).start()

    @pl.when(first)
    def _():
        for c in range(AHEAD):
            start_gather(c)

    late = s >= S // 2
    early = jnp.logical_not(late)

    @pl.when(late)
    def _():
        with scope("turn"):
            lax.fori_loop(0, T, turn_w, 0)

    def store_out(c, h):
        return pltpu.make_async_copy(outv.at[c, h], out_acts.at[c, :, pl.ds(h * C, C)], st_o)

    def forward(c, m):
        span = pl.ds(c, m)
        total = jnp.zeros((m * R, H * C), F32)
        for j in range(T):
            yb = at_y((2 * (1 - odd), 1, 3, 2 * odd)[j])

            def take():
                with scope(f"fwait{j}"):
                    for i in range(m):
                        wait_block(c + i, yb)

            if m > 1 or j < T - 1:
                take()
            else:
                pl.when(not_first)(take)

            for h in range(H):
                r = yb * H + h
                q = quantize(xg[span, r].reshape(m * R, C), act_factor, 448.0)
                xq[span, r] = q.reshape(m, R, C)
                total = total + jnp.dot(q, w[r], preferred_element_type=F32)
        for h in range(H):
            x = xg[span, y * H + h].reshape(m * R, C).astype(F32)
            o = x + total[:, h * C : (h + 1) * C] * forward_factor
            outv[span, h] = o.astype(BF16).reshape(m, R, C)

        def send():
            for i in range(m):
                for d in (2, 1, 3, 0):
                    out_copy(c + i, d).start()

        if m == 1:
            send()
        else:
            pl.when(not_last)(send)

        with scope("fz"):
            if m == 1:
                @pl.when(first & (c + AHEAD < n))
                def _():
                    start_gather(c + AHEAD)

            @pl.when(c // Q == y)
            def _():
                for d in (4, 3, 5, 2, 6, 1, 7):
                    act_copy(c, m, d).start()
                ar[span, z] = xq[span, z]

            for h in range(H):
                for i in range(m):
                    store_out(c + i, h).start()
                x = xg[span, y * H + h].reshape(m * R, C).astype(F32)
                amax[h] = jnp.maximum(amax[h], jnp.max(jnp.abs(x), axis=0, keepdims=True))

    side = first.astype(jnp.int32)

    def part_copy(c, d):
        yb = at_y(d)
        recv = p_recv.at[jnp.where(first, n, c)]
        return rcopy(ps.at[c, yb], pr.at[side, c, y], p_send, recv, pipe=down, tensor=yb)

    def back_copy(c):
        return rcopy(gin.at[c], gout.at[c], go_send, go_recv, pipe=up)

    def ring_copy(u, back):
        span = pl.ds(2 * u, 2)
        return rcopy(gq.at[span], gr.at[span, z], z_send, zr_recv.at[u, 3 * back], dp=at_z(Z - 1 if back else 1))

    def relay_copy(u, level, back):
        k = at_z(level if back else Z - level)
        span = pl.ds(2 * u, 2)
        if level < 3:
            ref = gr.at[span, k]
            recv = zr_recv.at[u, 3 * back + level]
        else:
            half = H * C // 2
            ref = gr.at[span, k, :, pl.ds(half * back, half)]
            recv = zo_recv.at[u]
        return rcopy(ref, ref, z_send, recv, dp=at_z(Z - 1 if back else 1))

    lag = jnp.where(s < 2, 1, 2)

    def relays(t):
        for level in (1, 2, 3):
            u = t - lag * level

            @pl.when((u >= 0) & (u < U))
            def _():
                with scope(f"relay{level}"):
                    for back in (0, 1):
                        k = at_z(level if back else Z - level)
                        drain_recv(zr_recv.at[u, 3 * back + level - 1], gr.at[pl.ds(2 * u, 2), k])
                        relay_copy(u, level, back).start()

    def store_g(c):
        return pltpu.make_async_copy(gout.at[c], out_grads.at[c], st_g)

    @pl.when(last)
    def _():
        load_c.wait()

    def backward(c, m):
        span = pl.ds(c, m)
        def begin():
            for h in range(H):
                part = cotv[span, :, h * C : (h + 1) * C].astype(F32) * outv[span, h].astype(F32)
                gin[span, :, h * C : (h + 1) * C] = part.astype(BF16)

        def arrive():
            with scope("bwait"):
                for i in range(m):
                    drain_recv(p_recv.at[c + i], pr.at[0, c + i])
            for h in range(H):
                g = pr[0, span, 0, h].astype(F32)
                for k in range(1, T):
                    g = g + pr[0, span, k, h].astype(F32)
                gin[span, :, h * C : (h + 1) * C] = g.astype(BF16)

        if m > 1:
            pl.when(last)(begin)
            pl.when(not_last)(arrive)
        else:
            arrive()
        g = gin[span].reshape(m * R, H * C)
        q = quantize(g, grad_factor, 57344.0)
        gq[span] = q.reshape(m, R, H * C)
        for d in (2, 1, 3, 0):
            yb = at_y(d)
            part = jnp.dot(q, wt[yb], preferred_element_type=F32) * backward_factor
            if d == 0:
                part = part + g.astype(F32)
            for h in range(H):
                ps[span, yb, h] = part[:, h * C : (h + 1) * C].astype(BF16).reshape(m, R, C)
            if d:
                for i in range(m):
                    part_copy(c + i, d).start()

        def to_own():
            for i in range(m):
                part_copy(c + i, 0).start()

        if m > 1:
            to_own()

            @pl.when(not_last)
            def _():
                for i in range(m):
                    back_copy(c + i).start()
        else:
            pl.when(not_first)(to_own)
            back_copy(c).start()
        with scope("bz"):
            gmax[...] = jnp.maximum(gmax[...], jnp.max(jnp.abs(g.astype(F32)), axis=0, keepdims=True))
            gr[span, z] = q.reshape(m, R, H * C)

    prior = s == S - 2
    inner = not_last & jnp.logical_not(prior)
    warm = jnp.where(last, 0, jnp.where(prior, WARM, n))

    def slot(k, u):
        ahead = k < warm
        pairs = jnp.logical_not(ahead) & jnp.logical_not(inner)
        late_k = k - warm
        mixed = jnp.logical_not(ahead) & (late_k < n - warm)
        turn = lax.rem(late_k, 2)
        fwd_pair = pairs & mixed & jnp.where(last, turn == 0, turn == 1)
        bwd_pair = pairs & jnp.logical_not(fwd_pair)
        bwd_one = jnp.logical_not(ahead) & inner
        f_at = warm + 2 * (late_k // 2)
        b_at = jnp.where(mixed, 2 * (late_k // 2), n - warm + 2 * (late_k - (n - warm)))

        @pl.when(ahead)
        def _():
            forward(k, 1)

        @pl.when(fwd_pair)
        def _():
            forward(f_at, 2)

        @pl.when(bwd_pair)
        def _():
            backward(b_at, 2)

        @pl.when(bwd_one)
        def _():
            backward(late_k, 1)

        unit = jnp.where(inner, late_k, b_at) // 2

        @pl.when(bwd_pair | (bwd_one & (lax.rem(late_k, 2) == 1)))
        def _():
            ring_copy(unit, 0).start()
            ring_copy(unit, 1).start()
            relays(unit)

        @pl.when(early & (k == n - 1))
        def _():
            with scope("turn"):
                lax.fori_loop(0, T, turn_w, 0)
            share_acts()

        return u

    lax.fori_loop(0, jnp.where(inner, 2 * n, jnp.where(last, n, n + WARM // 2)), slot, 0)

    lanes = pks.shape[-1]
    peak_a = jnp.max(jnp.maximum(amax[0], amax[H - 1]), axis=1, keepdims=True)
    peak_w = jnp.max(wmax[...], axis=1, keepdims=True)
    peak_g = jnp.max(gmax[...], axis=1, keepdims=True)
    row = lax.broadcasted_iota(jnp.int32, (8, lanes), 0)
    tile = jnp.where(row == 0, peak_a, jnp.where(row == 1, peak_w, peak_g))
    pks[...] = tile

    def ky_copy(d):
        return rcopy(pks, pky.at[y], ky_send, ky_recv, tensor=at_y(d))

    def kz_copy(d):
        return rcopy(pkm, pkz.at[z], kz_send, kz_recv, dp=at_z(d))

    for d in range(1, T):
        ky_copy(d).start()

    def rows_product(lo, count):
        left = ar[lo : lo + count].reshape(count * Z * R, C)
        right = gr[lo : lo + count].reshape(count * Z * R, H * C)
        return lax.dot_general(left, right, (((0,), (0,)), ((), ())), preferred_element_type=F32)

    def wait_opposite(lo, hi):
        for u in range(lo, hi):
            drain_recv(zo_recv.at[u], gr.at[pl.ds(2 * u, 2), 0])

    def first_rows():
        with scope("wgrad"):
            drain_recv(ay_recv, ar.at[pl.ds(0, (T - 1) * Q)])
            wait_opposite(0, U // 2)
            acc[...] = rows_product(0, n // 2)

    def rest(k, u):
        relays(k)

        @pl.when(late & (k == U + 1))
        def _():
            share_acts()

        @pl.when(early & (k == U - 1 + lag))
        def _():
            first_rows()

        return u

    lax.fori_loop(U, U + 3 * lag, rest, 0)

    with scope("kwait"):
        drain_recv(ky_recv, pky.at[pl.ds(0, T - 1)])
    pky[y] = tile
    for k in range(T):
        tile = jnp.maximum(tile, pky[k])
    pkm[...] = tile
    for d in range(1, Z):
        kz_copy(d).start()

    @pl.when(first)
    def _():
        def finish(c, u):
            for h in range(H):
                g = ps[c, y, h].astype(F32)
                for d in range(1, T):
                    g = g + pr[1, c, at_y(d), h].astype(F32)
                gout[c, :, h * C : (h + 1) * C] = g.astype(BF16)
            return u

        with scope("first"):
            drain_recv(p_recv.at[n], pr.at[1, :, pl.ds(0, T - 1)])
            lax.fori_loop(0, n, finish, 0)

    @pl.when(not_first)
    def _():
        with scope("backwait"):
            drain_recv(go_recv, gout)

    lax.fori_loop(0, n, lambda c, u: (store_g(c).start(), u)[1], 0)

    pl.when(late)(first_rows)
    with scope("wgrad2"):
        wait_opposite(U // 2, U - 1)
        acc[...] += rows_product(n // 2, n // 2 - 2)
    with scope("zwait_last"):
        wait_opposite(U - 1, U)
    with scope("wgrad_last"):
        wg[...] = ((acc[...] + rows_product(n - 2, 2)) * update_factor).astype(BF16)
    st = pltpu.make_async_copy(wg, out_wgrad, st_w)
    st.start()

    drain_recv(kz_recv, pkz.at[pl.ds(0, Z - 1)])
    pkz[z] = tile
    for k in range(Z):
        tile = jnp.maximum(tile, pkz[k])
    out_peaks[...] = tile

    with scope("close"):
        drain_send(ky_send, pky.at[pl.ds(0, T - 1)])
        drain_send(kz_send, pkz.at[pl.ds(0, Z - 1)])
        drain_send(a_send, ar.at[pl.ds(0, Q), pl.ds(0, Z - 1)])
        drain_send(ay_send, ar.at[pl.ds(0, (T - 1) * Q)])
        drain_send(z_send, gr.at[:, pl.ds(0, Z - 1)])

        @pl.when(first)
        def _():
            drain_send(fg_send, pr.at[0, :, pl.ds(0, T - 1)])
            drain_send(p_send, pr.at[0, :, pl.ds(0, T - 1)])

        @pl.when(not_first)
        def _():
            drain_send(p_send, pr.at[0])

        @pl.when(not_last)
        def _():
            drain_send(fo_send, pr.at[0])
            drain_send(go_send, gin)

        pltpu.make_async_copy(outv, outv, st_o).wait()
        pltpu.make_async_copy(gout, gout, st_g).wait()
        st.wait()


def finish_kernel(a, g, m, peaks, ha, hw, hg, oa, og, om, na, nw, ng, va, vg, vm, load, store):
    loads = [pltpu.make_async_copy(x, v, load.at[i]) for i, (x, v) in enumerate(((a, va), (g, vg), (m, vm)))]
    stores = [pltpu.make_async_copy(v, o, store.at[i]) for i, (v, o) in enumerate(((va, oa), (vg, og), (vm, om)))]
    for c in loads:
        c.start()
    for i, (old, new) in enumerate(((ha, na), (hw, nw), (hg, ng))):
        new[:, 1:] = old[:, :-1]
        new[:, 0:1] = peaks[i : i + 1, 0:1]
    for c, d in zip(loads, stores):
        c.wait()
        d.start()
    for d in stores:
        d.wait()


def step(acts_in, weights, cotangent, hist_act, hist_weight, hist_grad):
    S, Z, T = (lax.axis_size(a) for a in ("pipe", "dp", "tensor"))
    micro, rows, width = acts_in.shape
    depth = weights.shape[1]
    R = min(CHUNK, rows)
    n = micro * rows // R
    H = Z // T
    C = depth // Z
    acts = acts_in.reshape(n, R, width)
    cot = cotangent.reshape(n, R, width)
    w = weights.reshape(Z, C, width)
    any_ = pl.BlockSpec(memory_space=pl.ANY)
    hbm = pl.BlockSpec(memory_space=pltpu.HBM)
    vmem = pl.BlockSpec(memory_space=pltpu.VMEM)
    dma = pltpu.SemaphoreType.DMA
    b = lambda *shape: pltpu.VMEM(shape, BF16)
    f = lambda *shape: pltpu.VMEM(shape, F32)
    out_acts, out_grads, out_w, peaks = pl.pallas_call(
        functools.partial(kernel, S, Z, T, n, R),
        out_shape=(
            jax.ShapeDtypeStruct((n, R, width), BF16),
            jax.ShapeDtypeStruct((n, R, width), BF16),
            jax.ShapeDtypeStruct((C, width), BF16),
            jax.ShapeDtypeStruct((8, 128), F32),
        ),
        in_specs=[any_, any_, any_, vmem, vmem, vmem],
        out_specs=(any_, any_, any_, vmem),
        scratch_shapes=[
            b(Z, C, width), b(T, width, width), b(n, Z, R, C), b(n, Z, R, C), b(n, Z, R, C), b(n, Z, R, width),
            b(n, H, R, C), b(n, R, width), b(n, R, width), b(n, R, width),
            b(n, T, H, R, C), b(2, n, T, H, R, C), b(n, R, width), f(C, width),
            b(C, width), f(H, 1, C), f(1, width), f(1, width),
            f(8, 128), f(T, 8, 128), f(8, 128), f(Z, 8, 128),
            dma((Z,)), *(dma,) * 5,
            dma((n, T)), *(dma,) * 7, dma((n + 1,)), dma, dma, dma, dma((n // 2, 6)), dma((n // 2,)),
            *(dma,) * 4,
        ],
        compiler_params=pltpu.CompilerParams(
            collective_id=0, has_side_effects=True, vmem_limit_bytes=60 * 1024 * 1024
        ),
    )(acts, w, cot, hist_act, hist_weight, hist_grad)

    final = pl.pallas_call(
        finish_kernel,
        out_shape=(
            jax.ShapeDtypeStruct((n, R, width), BF16),
            jax.ShapeDtypeStruct((n, R, width), BF16),
            jax.ShapeDtypeStruct((C, width), BF16),
            *(jax.ShapeDtypeStruct(hist_act.shape, F32) for _ in range(3)),
        ),
        in_specs=[hbm, hbm, hbm, vmem, vmem, vmem, vmem],
        out_specs=(hbm, hbm, hbm, vmem, vmem, vmem),
        scratch_shapes=[b(n, R, width), b(n, R, width), b(C, width), dma((3,)), dma((3,))],
        compiler_params=pltpu.CompilerParams(vmem_limit_bytes=60 * 1024 * 1024),
    )(out_acts, out_grads, out_w, peaks, hist_act, hist_weight, hist_grad)
    return (
        final[0].reshape(1, micro, rows, width),
        final[1].reshape(1, micro, rows, width),
        final[2][None],
        *final[3:],
    )


def solution(mesh):
    placed = (
        P(None, "dp", "tensor"),
        P("pipe", None, "tensor"),
        P(None, "dp", "tensor"),
        P("pipe", None),
        P("pipe", None),
        P("pipe", None),
    )
    return jax.shard_map(
        step,
        mesh=mesh,
        in_specs=placed,
        out_specs=(
            P("pipe", None, "dp", "tensor"),
            P("pipe", None, "dp", "tensor"),
            P("pipe", "dp", "tensor"),
            P("pipe", None),
            P("pipe", None),
            P("pipe", None),
        ),
        check_vma=False,
    )
```

```python
import contextlib
import functools

import jax
import jax.numpy as jnp
from jax import lax
from jax.experimental import pallas as pl
from jax.experimental.pallas import tpu as pltpu
from jax.sharding import PartitionSpec as P

MESH = pl.DeviceIdType.MESH
F32 = jnp.float32
BF16 = jnp.bfloat16
CHUNK = 16
AHEAD = 5
WARM = 10

scope = lambda name: contextlib.nullcontext()


def quantize(values, factor, limit):
    return jnp.clip(values.astype(F32) * factor, -limit, limit).astype(BF16)


def gray(j):
    return j ^ (j >> 1)


def kernel(
    S, Z, T, n, R,
    acts, weights, cot, hist_act, hist_weight, hist_grad,
    out_acts, out_grads, out_wgrad, out_peaks,
    w, wt, xg, xq, ar, gr, outv, gin, gout, gq, ps, pr, cotv, acc, amax, wmax, gmax, pks, pky, pkm, pkz,
    ld_w, ld_x, ld_c,
    f_recv, fg_send, fo_send, a_send, a_recv, ay_send, ay_recv, p_send, p_recv, go_send, go_recv,
    z_send, zr_recv, zo_recv,
    ky_send, ky_recv, kz_send, kz_recv, far, hist, ld_h,
):
    s = lax.axis_index("pipe")
    z = lax.axis_index("dp")
    y = lax.axis_index("tensor")
    H = Z // T
    C = w.shape[1]
    U = n // 2
    Q = n // T
    odd = lax.rem(s, 2)
    even = odd == 0
    is_odd = odd == 1
    first = s == 0
    last = s == S - 1
    not_last = jnp.logical_not(last)
    not_first = jnp.logical_not(first)
    up = jnp.minimum(s + 1, S - 1)
    down = jnp.maximum(s - 1, 0)

    def at_y(d):
        return lax.rem(y + d, T)

    def at_z(d):
        return lax.rem(z + d, Z)

    def rcopy(src, dst, send, recv, **device):
        return pltpu.make_async_remote_copy(
            src_ref=src, dst_ref=dst, send_sem=send, recv_sem=recv, device_id=device, device_id_type=MESH
        )

    def drain_send(sem, ref):
        rcopy(ref, ref, sem, sem, tensor=at_y(1)).wait_send()

    def drain_recv(sem, ref):
        rcopy(ref, ref, sem, sem, tensor=at_y(1)).wait_recv()

    barrier = pltpu.get_barrier_semaphore()
    for d in range(1, T):
        pl.semaphore_signal(barrier, inc=1, device_id={"tensor": at_y(d)}, device_id_type=MESH)
    for d in (1, Z - 1):
        pl.semaphore_signal(barrier, inc=1, device_id={"dp": at_z(d)}, device_id_type=MESH)
    for d in range(T):
        @pl.when(not_last)
        def _():
            pl.semaphore_signal(barrier, inc=1, device_id={"pipe": up, "tensor": at_y(d)}, device_id_type=MESH)

        @pl.when(not_first)
        def _():
            pl.semaphore_signal(barrier, inc=1, device_id={"pipe": down, "tensor": at_y(d)}, device_id_type=MESH)

    own = pl.ds(y * H, H)

    def load_w(r):
        return pltpu.make_async_copy(weights.at[r], w.at[r], ld_w.at[r])

    def load_x(h):
        return pltpu.make_async_copy(acts.at[:, :, pl.ds(h * C, C)], xg.at[:, y * H + h], ld_x)

    load_c = pltpu.make_async_copy(cot, cotv, ld_c)
    load_h = [
        pltpu.make_async_copy(old, hist.at[i], ld_h.at[i])
        for i, old in enumerate((hist_act, hist_weight, hist_grad))
    ]
    for load in load_h:
        load.start()

    @pl.when(first)
    def _():
        for h in range(H):
            load_x(h).start()

    lax.fori_loop(0, Z, lambda r, u: (load_w(r).start(), u)[1], 0)

    @pl.when(last)
    def _():
        load_c.start()

    for load in load_h:
        load.wait()
    ha = jnp.max(hist[0], axis=1, keepdims=True)
    hw = jnp.max(hist[1], axis=1, keepdims=True)
    hg = jnp.max(hist[2], axis=1, keepdims=True)
    act_factor = 448.0 / ha
    weight_factor = 448.0 / hw
    grad_factor = 57344.0 / hg
    forward_factor = 1.0 / (act_factor * weight_factor)
    backward_factor = 1.0 / (grad_factor * weight_factor)
    update_factor = 1.0 / (act_factor * grad_factor)

    amax[...] = jnp.zeros_like(amax)
    wmax[...] = jnp.zeros_like(wmax)
    gmax[...] = jnp.zeros_like(gmax)

    @pl.when(first)
    def _():
        pltpu.make_async_copy(xg.at[:, own], xg.at[:, own], ld_x).wait()


    def gather_copy(c, d):
        return rcopy(xg.at[c, own], xg.at[c, own], fg_send, f_recv.at[c, y], tensor=at_y(d))

    def out_copy(c, d):
        return rcopy(outv.at[c], xg.at[c, own], fo_send, f_recv.at[c, y], pipe=up, tensor=at_y(d))

    def wait_block(c, yb):
        drain_recv(f_recv.at[c, yb], xg.at[c, pl.ds(yb * H, H)])

    def act_copy(c, m, d):
        r = at_z(d)
        span = pl.ds(c, m)
        return rcopy(xq.at[span, r], ar.at[span, z], a_send, a_recv, dp=r)

    def share_copy(d):
        span = pl.ds(y * Q, Q)
        return rcopy(ar.at[span], ar.at[span], ay_send, ay_recv, tensor=at_y(d))

    def share_acts():
        with scope("share"):
            drain_recv(a_recv, ar.at[pl.ds(0, Q), pl.ds(0, Z - 1)])
            for d in (2, 1, 3):
                share_copy(d).start()

    def quant_w(r, u):
        load_w(r).wait()
        raw = w[r].astype(F32)
        wmax[...] = jnp.maximum(wmax[...], jnp.max(jnp.abs(raw), axis=0, keepdims=True))
        w[r] = jnp.clip(raw * weight_factor, -448.0, 448.0).astype(BF16)
        return u

    def turn_w(k, u):
        for h in range(H):
            wt[k, :, h * C : (h + 1) * C] = w[k * H + h].T
        return u

    with scope("qw"):
        lax.fori_loop(0, Z, quant_w, 0)

    with scope("barrier"):
        pairs = not_first.astype(jnp.int32) + not_last.astype(jnp.int32)
        pl.semaphore_wait(barrier, (T - 1) + 2 + T * pairs)

    def start_gather(c):
        for d in (2, 1, 3):
            gather_copy(c, d).start()

    @pl.when(first)
    def _():
        for c in range(AHEAD):
            start_gather(c)

    def far_signal(level):
        for to in (level + 1, Z - 1 - level):
            pl.semaphore_signal(far.at[level], inc=1, device_id={"dp": at_z(to)}, device_id_type=MESH)

    far_signal(0)

    late = s >= S // 2
    early = jnp.logical_not(late)

    @pl.when(late)
    def _():
        with scope("turn"):
            lax.fori_loop(0, T, turn_w, 0)

    with scope("far0"):
        pl.semaphore_wait(far.at[0], 2)
        far_signal(1)

    def forward(c, m):
        span = pl.ds(c, m)
        total = jnp.zeros((m * R, H * C), F32)
        for j in range(T):
            yb = at_y((2 * (1 - odd), 1, 3, 2 * odd)[j])

            def take():
                with scope(f"fwait{j}"):
                    for i in range(m):
                        wait_block(c + i, yb)

            if m > 1 or j < T - 1:
                take()
            else:
                pl.when(not_first)(take)

            for h in range(H):
                r = yb * H + h
                q = quantize(xg[span, r].reshape(m * R, C), act_factor, 448.0)
                xq[span, r] = q.reshape(m, R, C)
                total = total + jnp.dot(q, w[r], preferred_element_type=F32)
        for h in range(H):
            x = xg[span, y * H + h].reshape(m * R, C).astype(F32)
            o = x + total[:, h * C : (h + 1) * C] * forward_factor
            outv[span, h] = o.astype(BF16).reshape(m, R, C)

        def send():
            for i in range(m):
                for d in (2, 1, 3, 0):
                    out_copy(c + i, d).start()

        if m == 1:
            send()
        else:
            pl.when(not_last)(send)

        with scope("fz"):
            if m == 1:
                @pl.when(first & (c + AHEAD < n))
                def _():
                    start_gather(c + AHEAD)

            @pl.when(c == 0)
            def _():
                pl.semaphore_wait(far.at[1], 2)

            @pl.when(c // Q == y)
            def _():
                for d in (4, 3, 5, 2, 6, 1, 7):
                    act_copy(c, m, d).start()
                ar[span, z] = xq[span, z]

            for h in range(H):
                out_acts[span, :, h * C : (h + 1) * C] = outv[span, h]
                x = xg[span, y * H + h].reshape(m * R, C).astype(F32)
                amax[h] = jnp.maximum(amax[h], jnp.max(jnp.abs(x), axis=0, keepdims=True))

    side = first.astype(jnp.int32)

    def part_copy(c, d):
        yb = at_y(d)
        recv = p_recv.at[jnp.where(first, n, c)]
        return rcopy(ps.at[c, yb], pr.at[side, c, y], p_send, recv, pipe=down, tensor=yb)

    def back_copy(c):
        return rcopy(gin.at[c], gout.at[c], go_send, go_recv, pipe=up)

    def ring_copy(u, back):
        span = pl.ds(2 * u, 2)
        return rcopy(gq.at[span], gr.at[span, z], z_send, zr_recv.at[u, 3 * back], dp=at_z(Z - 1 if back else 1))

    def relay_copy(u, level, back):
        k = at_z(level if back else Z - level)
        span = pl.ds(2 * u, 2)
        if level < 3:
            ref = gr.at[span, k]
            recv = zr_recv.at[u, 3 * back + level]
        else:
            half = H * C // 2
            ref = gr.at[span, k, :, pl.ds(half * back, half)]
            recv = zo_recv.at[u]
        return rcopy(ref, ref, z_send, recv, dp=at_z(Z - 1 if back else 1))

    lag = jnp.where(s < 2, 1, jnp.where(s < S - 2, 3, 4))

    def skip_copy(u, back):
        span = pl.ds(2 * u, 2)
        return rcopy(gq.at[span], gr.at[span, z], z_send, zr_recv.at[u, 3 * back + 1], dp=at_z(Z - 2 if back else 2))

    def over_copy(u, back):
        half = H * C // 2
        ref = gr.at[pl.ds(2 * u, 2), at_z(2 if back else Z - 2), :, pl.ds(half * back, half)]
        return rcopy(ref, ref, z_send, zo_recv.at[u], dp=at_z(Z - 2 if back else 2))

    def short(u):
        return first & (u == U - 1)

    def relays(t):
        for level in (1, 2, 3):
            u = t - lag * level

            @pl.when((u >= 0) & (u < U))
            def _():
                with scope(f"relay{level}"):
                    for back in (0, 1):
                        k = at_z(level if back else Z - level)
                        drain_recv(zr_recv.at[u, 3 * back + level - 1], gr.at[pl.ds(2 * u, 2), k])
                        if level == 2:
                            relay_copy(u, level, back).start()

                            @pl.when(short(u))
                            def _():
                                over_copy(u, back).start()
                        else:
                            @pl.when(jnp.logical_not(short(u)))
                            def _():
                                relay_copy(u, level, back).start()

    @pl.when(last)
    def _():
        load_c.wait()

    def backward(c, m):
        span = pl.ds(c, m)
        def begin():
            for h in range(H):
                part = cotv[span, :, h * C : (h + 1) * C].astype(F32) * outv[span, h].astype(F32)
                gin[span, :, h * C : (h + 1) * C] = part.astype(BF16)

        def arrive():
            with scope("bwait"):
                for i in range(m):
                    drain_recv(p_recv.at[c + i], pr.at[0, c + i])
            for h in range(H):
                g = pr[0, span, 0, h].astype(F32)
                for k in range(1, T):
                    g = g + pr[0, span, k, h].astype(F32)
                gin[span, :, h * C : (h + 1) * C] = g.astype(BF16)

        if m > 1:
            pl.when(last)(begin)
            pl.when(not_last)(arrive)
        else:
            arrive()
        g = gin[span].reshape(m * R, H * C)
        q = quantize(g, grad_factor, 57344.0)
        gq[span] = q.reshape(m, R, H * C)
        for d in (2, 1, 3, 0):
            yb = at_y(d)
            part = jnp.dot(q, wt[yb], preferred_element_type=F32) * backward_factor
            if d == 0:
                part = part + g.astype(F32)
            for h in range(H):
                ps[span, yb, h] = part[:, h * C : (h + 1) * C].astype(BF16).reshape(m, R, C)
            if d:
                for i in range(m):
                    part_copy(c + i, d).start()

        def to_own():
            for i in range(m):
                part_copy(c + i, 0).start()

        if m > 1:
            to_own()

            @pl.when(not_last)
            def _():
                for i in range(m):
                    back_copy(c + i).start()
        else:
            pl.when(not_first)(to_own)
            back_copy(c).start()
        with scope("bz"):
            gmax[...] = jnp.maximum(gmax[...], jnp.max(jnp.abs(g.astype(F32)), axis=0, keepdims=True))
            gr[span, z] = q.reshape(m, R, H * C)

    prior = s == S - 2
    inner = not_last & jnp.logical_not(prior)
    warm = jnp.where(last, 0, jnp.where(prior, WARM, n))

    def slot(k, u):
        ahead = k < warm
        pairs = jnp.logical_not(ahead) & jnp.logical_not(inner)
        late_k = k - warm
        mixed = jnp.logical_not(ahead) & (late_k < n - warm)
        turn = lax.rem(late_k, 2)
        fwd_pair = pairs & mixed & jnp.where(last, turn == 0, turn == 1)
        bwd_pair = pairs & jnp.logical_not(fwd_pair)
        bwd_one = jnp.logical_not(ahead) & inner
        f_at = warm + 2 * (late_k // 2)
        b_at = jnp.where(mixed, 2 * (late_k // 2), n - warm + 2 * (late_k - (n - warm)))

        @pl.when(ahead)
        def _():
            forward(k, 1)

        @pl.when(fwd_pair)
        def _():
            forward(f_at, 2)

        @pl.when(bwd_pair)
        def _():
            backward(b_at, 2)

        @pl.when(bwd_one)
        def _():
            backward(late_k, 1)

        unit = jnp.where(inner, late_k, b_at) // 2

        @pl.when(bwd_pair | (bwd_one & (lax.rem(late_k, 2) == 1)))
        def _():
            @pl.when(short(unit))
            def _():
                skip_copy(unit, 0).start()
                skip_copy(unit, 1).start()

            ring_copy(unit, 0).start()
            ring_copy(unit, 1).start()
            relays(unit)

        @pl.when(early & (k == n - 1))
        def _():
            with scope("turn"):
                lax.fori_loop(0, T, turn_w, 0)
            share_acts()

        return u

    lax.fori_loop(0, jnp.where(inner, 2 * n, jnp.where(last, n, n + WARM // 2)), slot, 0)

    lanes = pks.shape[-1]
    peak_a = jnp.max(jnp.maximum(amax[0], amax[H - 1]), axis=1, keepdims=True)
    peak_w = jnp.max(wmax[...], axis=1, keepdims=True)
    peak_g = jnp.max(gmax[...], axis=1, keepdims=True)
    row = lax.broadcasted_iota(jnp.int32, (8, lanes), 0)
    tile = jnp.where(row == 0, peak_a, jnp.where(row == 1, peak_w, peak_g))
    pks[...] = tile

    def ky_copy(d):
        return rcopy(pks, pky.at[y], ky_send, ky_recv, tensor=at_y(d))

    def kz_copy(d):
        return rcopy(pkm, pkz.at[z], kz_send, kz_recv, dp=at_z(d))

    for d in range(1, T):
        ky_copy(d).start()

    def over_tensor():
        with scope("kwait"):
            drain_recv(ky_recv, pky.at[pl.ds(0, T - 1)])
        pky[y] = pks[...]
        most = pky[0]
        for k in range(1, T):
            most = jnp.maximum(most, pky[k])
        pkm[...] = most
        for d in range(1, Z):
            kz_copy(d).start()

    def rows_product(lo, count):
        left = ar[lo : lo + count].reshape(count * Z * R, C)
        right = gr[lo : lo + count].reshape(count * Z * R, H * C)
        return lax.dot_general(left, right, (((0,), (0,)), ((), ())), preferred_element_type=F32)

    def wait_opposite(lo, hi):
        for u in range(lo, hi):
            drain_recv(zo_recv.at[u], gr.at[pl.ds(2 * u, 2), 0])

    def first_rows():
        with scope("wgrad"):
            drain_recv(ay_recv, ar.at[pl.ds(0, (T - 1) * Q)])
            wait_opposite(0, U // 2)
            acc[...] = rows_product(0, n // 2)

    def next_rows():
        with scope("wgrad2"):
            wait_opposite(U // 2, U - 2)
            acc[...] += rows_product(n // 2, n // 2 - 4)

    near = s < 2

    def rest(k, u):
        pl.when(early & (k == jnp.where(near, U, U + 5)))(first_rows)
        pl.when(near & (k == U + 2))(next_rows)
        relays(k)
        pl.when(k == U + 1)(over_tensor)

        @pl.when(late & (k == U + 2))
        def _():
            share_acts()

        return u

    yields = is_odd & (s > 1)

    @pl.when(yields)
    def _():
        with scope("yield"):
            drain_recv(go_recv, gout)

    lax.fori_loop(U, U + 3 * lag, rest, 0)

    @pl.when(first)
    def _():
        def finish(c, u):
            for h in range(H):
                g = ps[c, y, h].astype(F32)
                for d in range(1, T):
                    g = g + pr[1, c, at_y(d), h].astype(F32)
                gout[c, :, h * C : (h + 1) * C] = g.astype(BF16)
            return u

        with scope("first"):
            drain_recv(p_recv.at[n], pr.at[1, :, pl.ds(0, T - 1)])
            lax.fori_loop(0, n, finish, 0)

    @pl.when(not_first & jnp.logical_not(yields))
    def _():
        with scope("backwait"):
            drain_recv(go_recv, gout)

    out_grads[...] = gout[...]

    pl.when(late)(first_rows)
    pl.when(jnp.logical_not(near))(next_rows)
    with scope("zwait_last"):
        wait_opposite(U - 2, U)
    with scope("wgrad_last"):
        out_wgrad[...] = ((acc[...] + rows_product(n - 4, 4)) * update_factor).astype(BF16)

    drain_recv(kz_recv, pkz.at[pl.ds(0, Z - 1)])
    pkz[z] = pkm[...]
    most = pkz[0]
    for k in range(1, Z):
        most = jnp.maximum(most, pkz[k])
    out_peaks[...] = most

    with scope("close"):
        drain_send(ky_send, pky.at[pl.ds(0, T - 1)])
        drain_send(kz_send, pkz.at[pl.ds(0, Z - 1)])
        drain_send(a_send, ar.at[pl.ds(0, Q), pl.ds(0, Z - 1)])
        drain_send(ay_send, ar.at[pl.ds(0, (T - 1) * Q)])
        drain_send(z_send, gr.at[:, pl.ds(0, Z - 1)])

        @pl.when(first)
        def _():
            drain_send(fg_send, pr.at[0, :, pl.ds(0, T - 1)])
            drain_send(p_send, pr.at[0, :, pl.ds(0, T - 1)])

        @pl.when(not_first)
        def _():
            drain_send(p_send, pr.at[0])

        @pl.when(not_last)
        def _():
            drain_send(fo_send, pr.at[0])
            drain_send(go_send, gin)


def finish_kernel(a, g, m, peaks, ha, hw, hg, oa, og, om, na, nw, ng, store):
    stores = [pltpu.make_async_copy(v, o, store.at[i]) for i, (v, o) in enumerate(((a, oa), (g, og), (m, om)))]
    for d in stores:
        d.start()
    for i, (old, new) in enumerate(((ha, na), (hw, nw), (hg, ng))):
        new[:, 1:] = old[:, :-1]
        new[:, 0:1] = peaks[i : i + 1, 0:1]
    for d in stores:
        d.wait()


def step(acts_in, weights, cotangent, hist_act, hist_weight, hist_grad):
    S, Z, T = (lax.axis_size(a) for a in ("pipe", "dp", "tensor"))
    micro, rows, width = acts_in.shape
    depth = weights.shape[1]
    R = min(CHUNK, rows)
    n = micro * rows // R
    H = Z // T
    C = depth // Z
    acts = pltpu.with_memory_space_constraint(acts_in.reshape(n, R, width), pltpu.HBM)
    cot = pltpu.with_memory_space_constraint(cotangent.reshape(n, R, width), pltpu.HBM)
    w = weights.reshape(Z, C, width)
    any_ = pl.BlockSpec(memory_space=pl.ANY)
    hbm = pl.BlockSpec(memory_space=pltpu.HBM)
    vmem = pl.BlockSpec(memory_space=pltpu.VMEM)
    dma = pltpu.SemaphoreType.DMA
    b = lambda *shape: pltpu.VMEM(shape, BF16)
    f = lambda *shape: pltpu.VMEM(shape, F32)
    out_acts, out_grads, out_w, peaks = pl.pallas_call(
        functools.partial(kernel, S, Z, T, n, R),
        out_shape=(
            jax.ShapeDtypeStruct((n, R, width), BF16),
            jax.ShapeDtypeStruct((n, R, width), BF16),
            jax.ShapeDtypeStruct((C, width), BF16),
            jax.ShapeDtypeStruct((8, 128), F32),
        ),
        in_specs=[any_] * 6,
        out_specs=(vmem, vmem, vmem, vmem),
        scratch_shapes=[
            b(Z, C, width), b(T, width, width), b(n, Z, R, C), b(n, Z, R, C), b(n, Z, R, C), b(n, Z, R, width),
            b(n, H, R, C), b(n, R, width), b(n, R, width), b(n, R, width),
            b(n, T, H, R, C), b(2, n, T, H, R, C), b(n, R, width), f(C, width),
            f(H, 1, C), f(1, width), f(1, width),
            f(8, 128), f(T, 8, 128), f(8, 128), f(Z, 8, 128),
            dma((Z,)), dma, dma,
            dma((n, T)), *(dma,) * 7, dma((n + 1,)), dma, dma, dma, dma((n // 2, 6)), dma((n // 2,)),
            *(dma,) * 4, pltpu.SemaphoreType.REGULAR((2,)), f(3, *hist_act.shape), dma((3,)),
        ],
        compiler_params=pltpu.CompilerParams(
            collective_id=0, has_side_effects=True, vmem_limit_bytes=52000000
        ),
    )(acts, w, cot, *(pltpu.with_memory_space_constraint(h, pltpu.HBM) for h in (hist_act, hist_weight, hist_grad)))

    final = pl.pallas_call(
        finish_kernel,
        out_shape=(
            jax.ShapeDtypeStruct((n, R, width), BF16),
            jax.ShapeDtypeStruct((n, R, width), BF16),
            jax.ShapeDtypeStruct((C, width), BF16),
            *(jax.ShapeDtypeStruct(hist_act.shape, F32) for _ in range(3)),
        ),
        in_specs=[vmem] * 7,
        out_specs=(hbm, hbm, hbm, vmem, vmem, vmem),
        scratch_shapes=[dma((3,))],
        compiler_params=pltpu.CompilerParams(vmem_limit_bytes=8 * 1024 * 1024),
    )(out_acts, out_grads, out_w, peaks, hist_act, hist_weight, hist_grad)
    return (
        final[0].reshape(1, micro, rows, width),
        final[1].reshape(1, micro, rows, width),
        final[2][None],
        *final[3:],
    )


def solution(mesh):
    placed = (
        P(None, "dp", "tensor"),
        P("pipe", None, "tensor"),
        P(None, "dp", "tensor"),
        P("pipe", None),
        P("pipe", None),
        P("pipe", None),
    )
    return jax.shard_map(
        step,
        mesh=mesh,
        in_specs=placed,
        out_specs=(
            P("pipe", None, "dp", "tensor"),
            P("pipe", None, "dp", "tensor"),
            P("pipe", "dp", "tensor"),
            P("pipe", None),
            P("pipe", None),
            P("pipe", None),
        ),
        check_vma=False,
    )
```

```python
import contextlib
import functools

import jax
import jax.numpy as jnp
from jax import lax
from jax.experimental import pallas as pl
from jax.experimental.pallas import tpu as pltpu
from jax.sharding import PartitionSpec as P

MESH = pl.DeviceIdType.MESH
F32 = jnp.float32
BF16 = jnp.bfloat16
CHUNK = 16
AHEAD = 5
WARM = 10
LENT = 2

scope = lambda name: contextlib.nullcontext()


def quantize(values, factor, limit):
    return jnp.clip(values.astype(F32) * factor, -limit, limit).astype(BF16)


def gray(j):
    return j ^ (j >> 1)


def kernel(
    S, Z, T, n, R,
    acts, weights, cot, hist_act, hist_weight, hist_grad,
    out_acts, out_grads, out_wgrad, out_peaks,
    w, wt, xg, xq, ar, gr, outv, gin, gout, gq, ps, pr, cotv, hb, acc, amax, wmax, gmax, pks, pky, pkm, pkz,
    ld_w, ld_x, ld_c,
    f_recv, fg_send, fo_send, a_send, a_recv, ay_send, ay_recv, p_send, p_recv, go_send, go_recv,
    z_send, zr_recv, zo_recv,
    h_send, h_recv, hz_send, hr_recv, ho_recv, hx_send, hx_recv,
    ky_send, ky_recv, kz_send, kz_recv, far, hist, ld_h,
):
    s = lax.axis_index("pipe")
    z = lax.axis_index("dp")
    y = lax.axis_index("tensor")
    H = Z // T
    C = w.shape[1]
    U = n // 2
    Q = n // T
    odd = lax.rem(s, 2)
    even = odd == 0
    is_odd = odd == 1
    first = s == 0
    last = s == S - 1
    not_last = jnp.logical_not(last)
    near = s < 2
    helper = s >= S - 2
    buddy = jnp.where(near, s + S - 2, jnp.maximum(s - (S - 2), 0))
    not_first = jnp.logical_not(first)
    up = jnp.minimum(s + 1, S - 1)
    down = jnp.maximum(s - 1, 0)

    def at_y(d):
        return lax.rem(y + d, T)

    def at_z(d):
        return lax.rem(z + d, Z)

    def rcopy(src, dst, send, recv, **device):
        return pltpu.make_async_remote_copy(
            src_ref=src, dst_ref=dst, send_sem=send, recv_sem=recv, device_id=device, device_id_type=MESH
        )

    def drain_send(sem, ref):
        rcopy(ref, ref, sem, sem, tensor=at_y(1)).wait_send()

    def drain_recv(sem, ref):
        rcopy(ref, ref, sem, sem, tensor=at_y(1)).wait_recv()

    barrier = pltpu.get_barrier_semaphore()
    for d in range(1, T):
        pl.semaphore_signal(barrier, inc=1, device_id={"tensor": at_y(d)}, device_id_type=MESH)
    for d in (1, Z - 1):
        pl.semaphore_signal(barrier, inc=1, device_id={"dp": at_z(d)}, device_id_type=MESH)
    for d in range(T):
        @pl.when(not_last)
        def _():
            pl.semaphore_signal(barrier, inc=1, device_id={"pipe": up, "tensor": at_y(d)}, device_id_type=MESH)

        @pl.when(not_first)
        def _():
            pl.semaphore_signal(barrier, inc=1, device_id={"pipe": down, "tensor": at_y(d)}, device_id_type=MESH)

    @pl.when(near | helper)
    def _():
        pl.semaphore_signal(barrier, inc=1, device_id={"pipe": buddy}, device_id_type=MESH)

    own = pl.ds(y * H, H)

    def load_w(r):
        return pltpu.make_async_copy(weights.at[r], w.at[r], ld_w.at[r])

    def load_x(h):
        return pltpu.make_async_copy(acts.at[:, :, pl.ds(h * C, C)], xg.at[:, y * H + h], ld_x)

    load_c = pltpu.make_async_copy(cot, cotv, ld_c)
    load_h = [
        pltpu.make_async_copy(old, hist.at[i], ld_h.at[i])
        for i, old in enumerate((hist_act, hist_weight, hist_grad))
    ]
    for load in load_h:
        load.start()

    @pl.when(first)
    def _():
        for h in range(H):
            load_x(h).start()

    lax.fori_loop(0, Z, lambda r, u: (load_w(r).start(), u)[1], 0)

    @pl.when(last)
    def _():
        load_c.start()

    for load in load_h:
        load.wait()
    ha = jnp.max(hist[0], axis=1, keepdims=True)
    hw = jnp.max(hist[1], axis=1, keepdims=True)
    hg = jnp.max(hist[2], axis=1, keepdims=True)
    act_factor = 448.0 / ha
    weight_factor = 448.0 / hw
    grad_factor = 57344.0 / hg
    forward_factor = 1.0 / (act_factor * weight_factor)
    backward_factor = 1.0 / (grad_factor * weight_factor)
    update_factor = 1.0 / (act_factor * grad_factor)

    amax[...] = jnp.zeros_like(amax)
    wmax[...] = jnp.zeros_like(wmax)
    gmax[...] = jnp.zeros_like(gmax)

    @pl.when(first)
    def _():
        pltpu.make_async_copy(xg.at[:, own], xg.at[:, own], ld_x).wait()


    def gather_copy(c, d):
        return rcopy(xg.at[c, own], xg.at[c, own], fg_send, f_recv.at[c, y], tensor=at_y(d))

    def out_copy(c, d):
        return rcopy(outv.at[c], xg.at[c, own], fo_send, f_recv.at[c, y], pipe=up, tensor=at_y(d))

    def wait_block(c, yb):
        drain_recv(f_recv.at[c, yb], xg.at[c, pl.ds(yb * H, H)])

    def act_copy(c, m, d):
        r = at_z(d)
        span = pl.ds(c, m)
        return rcopy(xq.at[span, r], ar.at[span, z], a_send, a_recv, dp=r)

    def share_copy(d, j):
        span = pl.ds(2 * (y + T * j), 2)
        return rcopy(ar.at[span], ar.at[span], ay_send, ay_recv, tensor=at_y(d))

    def share_acts():
        with scope("share"):
            drain_recv(a_recv, ar.at[pl.ds(0, Q), pl.ds(0, Z - 1)])
            for j in range(U // T):
                for d in (2, 1, 3):
                    share_copy(d, j).start()

    def quant_w(r, u):
        load_w(r).wait()
        raw = w[r].astype(F32)
        wmax[...] = jnp.maximum(wmax[...], jnp.max(jnp.abs(raw), axis=0, keepdims=True))
        w[r] = jnp.clip(raw * weight_factor, -448.0, 448.0).astype(BF16)
        return u

    def turn_w(k, u):
        for h in range(H):
            wt[k, :, h * C : (h + 1) * C] = w[k * H + h].T
        return u

    with scope("qw"):
        lax.fori_loop(0, Z, quant_w, 0)

    with scope("barrier"):
        pairs = not_first.astype(jnp.int32) + not_last.astype(jnp.int32)
        pl.semaphore_wait(barrier, (T - 1) + 2 + T * pairs + (near | helper).astype(jnp.int32))

    def start_gather(c):
        for d in (2, 1, 3):
            gather_copy(c, d).start()

    @pl.when(first)
    def _():
        for c in range(AHEAD):
            start_gather(c)

    def far_signal(level):
        for to in (level + 1, Z - 1 - level):
            pl.semaphore_signal(far.at[level], inc=1, device_id={"dp": at_z(to)}, device_id_type=MESH)

    far_signal(0)

    late = s >= S // 2
    early = jnp.logical_not(late)

    @pl.when(late)
    def _():
        with scope("turn"):
            lax.fori_loop(0, T, turn_w, 0)

    with scope("far0"):
        pl.semaphore_wait(far.at[0], 2)
        far_signal(1)

    def forward(c, m):
        span = pl.ds(c, m)
        total = jnp.zeros((m * R, H * C), F32)
        for j in range(T):
            yb = at_y((2 * (1 - odd), 1, 3, 2 * odd)[j])

            def take():
                with scope(f"fwait{j}"):
                    for i in range(m):
                        wait_block(c + i, yb)

            if m > 1 or j < T - 1:
                take()
            else:
                pl.when(not_first)(take)

            for h in range(H):
                r = yb * H + h
                q = quantize(xg[span, r].reshape(m * R, C), act_factor, 448.0)
                xq[span, r] = q.reshape(m, R, C)
                total = total + jnp.dot(q, w[r], preferred_element_type=F32)
        for h in range(H):
            x = xg[span, y * H + h].reshape(m * R, C).astype(F32)
            o = x + total[:, h * C : (h + 1) * C] * forward_factor
            outv[span, h] = o.astype(BF16).reshape(m, R, C)

        def send():
            for i in range(m):
                for d in (2, 1, 3, 0):
                    out_copy(c + i, d).start()

        if m == 1:
            send()
        else:
            pl.when(not_last)(send)

        with scope("fz"):
            if m == 1:
                @pl.when(first & (c + AHEAD < n))
                def _():
                    start_gather(c + AHEAD)

            @pl.when(c == 0)
            def _():
                pl.semaphore_wait(far.at[1], 2)

            @pl.when(lax.rem(c // 2, T) == y)
            def _():
                for d in (4, 3, 5, 2, 6, 1, 7):
                    act_copy(c, m, d).start()
                ar[span, z] = xq[span, z]

            for h in range(H):
                out_acts[span, :, h * C : (h + 1) * C] = outv[span, h]
                x = xg[span, y * H + h].reshape(m * R, C).astype(F32)
                amax[h] = jnp.maximum(amax[h], jnp.max(jnp.abs(x), axis=0, keepdims=True))

    side = first.astype(jnp.int32)

    def part_copy(c, d):
        yb = at_y(d)
        recv = p_recv.at[jnp.where(first, n, c)]
        return rcopy(ps.at[c, yb], pr.at[side, c, y], p_send, recv, pipe=down, tensor=yb)

    def back_copy(c):
        return rcopy(gin.at[c], gout.at[c], go_send, go_recv, pipe=up)

    def ring_copy(u, back):
        span = pl.ds(2 * u, 2)
        return rcopy(gq.at[span], gr.at[span, z], z_send, zr_recv.at[u, 3 * back], dp=at_z(Z - 1 if back else 1))

    def relay_copy(u, level, back):
        k = at_z(level if back else Z - level)
        span = pl.ds(2 * u, 2)
        if level < 3:
            ref = gr.at[span, k]
            recv = zr_recv.at[u, 3 * back + level]
        else:
            half = H * C // 2
            ref = gr.at[span, k, :, pl.ds(half * back, half)]
            recv = zo_recv.at[u]
        return rcopy(ref, ref, z_send, recv, dp=at_z(Z - 1 if back else 1))

    lag = jnp.where(s < 2, 1, 3)

    def skip_copy(u, back):
        span = pl.ds(2 * u, 2)
        return rcopy(gq.at[span], gr.at[span, z], z_send, zr_recv.at[u, 3 * back + 1], dp=at_z(Z - 2 if back else 2))

    def over_copy(u, back):
        half = H * C // 2
        ref = gr.at[pl.ds(2 * u, 2), at_z(2 if back else Z - 2), :, pl.ds(half * back, half)]
        return rcopy(ref, ref, z_send, zo_recv.at[u], dp=at_z(Z - 2 if back else 2))

    def lent(u):
        return near & (lax.rem(u, 2) == 1) & (u < 2 * LENT)

    def lend_copy(u):
        i = u // 2
        return rcopy(gq.at[pl.ds(2 * u, 2)], hb.at[pl.ds(2 * i, 2), z], h_send, h_recv.at[i], pipe=buddy)

    def help_copy(i, level, back):
        span = pl.ds(2 * i, 2)
        k = at_z(level if back else Z - level) if level else z
        if level < 3:
            ref, recv = hb.at[span, k], hr_recv.at[i, 3 * back + level]
        else:
            half = H * C // 2
            ref, recv = hb.at[span, k, :, pl.ds(half * back, half)], ho_recv.at[i]
        return rcopy(ref, ref, hz_send, recv, dp=at_z(Z - 1 if back else 1))

    def return_copy(i, k):
        return rcopy(hb.at[pl.ds(2 * i, 2), k], gr.at[pl.ds(4 * i + 2, 2), k], hx_send, hx_recv.at[i], pipe=buddy)

    def assist(t, v):
        for level in range(5):
            i = t - level

            @pl.when((i >= 0) & (i < LENT))
            def _():
                span = pl.ds(2 * i, 2)
                with scope(f"assist{level}"):
                    if level == 0:
                        drain_recv(h_recv.at[i], hb.at[span, z])
                        help_copy(i, 0, 0).start()
                        help_copy(i, 0, 1).start()
                    elif level < 4:
                        for back in (0, 1):
                            k = at_z(level if back else Z - level)
                            drain_recv(hr_recv.at[i, 3 * back + level - 1], hb.at[span, k])
                            help_copy(i, level, back).start()
                            return_copy(i, k).start()
                    else:
                        drain_recv(ho_recv.at[i], hb.at[span, at_z(4)])
                        return_copy(i, at_z(4)).start()

        return v

    def short(u):
        return first & (u == U - 1)

    def relays(t):
        for level in (1, 2, 3):
            u = t - lag * level

            @pl.when((u >= 0) & (u < U) & jnp.logical_not(lent(u)))
            def _():
                with scope(f"relay{level}"):
                    for back in (0, 1):
                        k = at_z(level if back else Z - level)
                        drain_recv(zr_recv.at[u, 3 * back + level - 1], gr.at[pl.ds(2 * u, 2), k])
                        if level == 2:
                            relay_copy(u, level, back).start()

                            @pl.when(short(u))
                            def _():
                                over_copy(u, back).start()
                        else:
                            @pl.when(jnp.logical_not(short(u)))
                            def _():
                                relay_copy(u, level, back).start()

    @pl.when(last)
    def _():
        load_c.wait()

    def backward(c, m):
        span = pl.ds(c, m)
        def begin():
            for h in range(H):
                part = cotv[span, :, h * C : (h + 1) * C].astype(F32) * outv[span, h].astype(F32)
                gin[span, :, h * C : (h + 1) * C] = part.astype(BF16)

        def arrive():
            with scope("bwait"):
                for i in range(m):
                    drain_recv(p_recv.at[c + i], pr.at[0, c + i])
            for h in range(H):
                g = pr[0, span, 0, h].astype(F32)
                for k in range(1, T):
                    g = g + pr[0, span, k, h].astype(F32)
                gin[span, :, h * C : (h + 1) * C] = g.astype(BF16)

        if m > 1:
            pl.when(last)(begin)
            pl.when(not_last)(arrive)
        else:
            arrive()
        g = gin[span].reshape(m * R, H * C)
        q = quantize(g, grad_factor, 57344.0)
        gq[span] = q.reshape(m, R, H * C)
        for d in (2, 1, 3, 0):
            yb = at_y(d)
            part = jnp.dot(q, wt[yb], preferred_element_type=F32) * backward_factor
            if d == 0:
                part = part + g.astype(F32)
            for h in range(H):
                ps[span, yb, h] = part[:, h * C : (h + 1) * C].astype(BF16).reshape(m, R, C)
            if d:
                for i in range(m):
                    part_copy(c + i, d).start()

        def to_own():
            for i in range(m):
                part_copy(c + i, 0).start()

        if m > 1:
            to_own()

            @pl.when(not_last)
            def _():
                for i in range(m):
                    back_copy(c + i).start()
        else:
            pl.when(not_first)(to_own)
            back_copy(c).start()
        with scope("bz"):
            gmax[...] = jnp.maximum(gmax[...], jnp.max(jnp.abs(g.astype(F32)), axis=0, keepdims=True))
            gr[span, z] = q.reshape(m, R, H * C)

    prior = s == S - 2
    inner = not_last & jnp.logical_not(prior)
    warm = jnp.where(last, 0, jnp.where(prior, WARM, n))

    def slot(k, u):
        ahead = k < warm
        pairs = jnp.logical_not(ahead) & jnp.logical_not(inner)
        late_k = k - warm
        mixed = jnp.logical_not(ahead) & (late_k < n - warm)
        turn = lax.rem(late_k, 2)
        fwd_pair = pairs & mixed & jnp.where(last, turn == 0, turn == 1)
        bwd_pair = pairs & jnp.logical_not(fwd_pair)
        bwd_one = jnp.logical_not(ahead) & inner
        f_at = warm + 2 * (late_k // 2)
        b_at = jnp.where(mixed, 2 * (late_k // 2), n - warm + 2 * (late_k - (n - warm)))

        @pl.when(ahead)
        def _():
            forward(k, 1)

        @pl.when(fwd_pair)
        def _():
            forward(f_at, 2)

        @pl.when(bwd_pair)
        def _():
            backward(b_at, 2)

        @pl.when(bwd_one)
        def _():
            backward(late_k, 1)

        unit = jnp.where(inner, late_k, b_at) // 2

        @pl.when(bwd_pair | (bwd_one & (lax.rem(late_k, 2) == 1)))
        def _():
            @pl.when(short(unit))
            def _():
                skip_copy(unit, 0).start()
                skip_copy(unit, 1).start()

            @pl.when(lent(unit))
            def _():
                lend_copy(unit).start()

            @pl.when(jnp.logical_not(lent(unit)))
            def _():
                ring_copy(unit, 0).start()
                ring_copy(unit, 1).start()

            relays(unit)

        @pl.when(early & (k == n - 1))
        def _():
            with scope("turn"):
                lax.fori_loop(0, T, turn_w, 0)
            share_acts()

        return u

    lax.fori_loop(0, jnp.where(inner, 2 * n, jnp.where(last, n, n + WARM // 2)), slot, 0)

    lanes = pks.shape[-1]
    peak_a = jnp.max(jnp.maximum(amax[0], amax[H - 1]), axis=1, keepdims=True)
    peak_w = jnp.max(wmax[...], axis=1, keepdims=True)
    peak_g = jnp.max(gmax[...], axis=1, keepdims=True)
    row = lax.broadcasted_iota(jnp.int32, (8, lanes), 0)
    tile = jnp.where(row == 0, peak_a, jnp.where(row == 1, peak_w, peak_g))
    pks[...] = tile

    def ky_copy(d):
        return rcopy(pks, pky.at[y], ky_send, ky_recv, tensor=at_y(d))

    def kz_copy(d):
        return rcopy(pkm, pkz.at[z], kz_send, kz_recv, dp=at_z(d))

    for d in range(1, T):
        ky_copy(d).start()

    def over_tensor():
        with scope("kwait"):
            drain_recv(ky_recv, pky.at[pl.ds(0, T - 1)])
        pky[y] = pks[...]
        most = pky[0]
        for k in range(1, T):
            most = jnp.maximum(most, pky[k])
        pkm[...] = most
        for d in range(1, Z):
            kz_copy(d).start()

    def rows_product(lo, count):
        left = ar[lo : lo + count].reshape(count * Z * R, C)
        right = gr[lo : lo + count].reshape(count * Z * R, H * C)
        return lax.dot_general(left, right, (((0,), (0,)), ((), ())), preferred_element_type=F32)

    def wait_opposite(lo, hi):
        for u in range(lo, hi):
            def own_ring():
                drain_recv(zo_recv.at[u], gr.at[pl.ds(2 * u, 2), 0])

            if u % 2 == 1 and u < 2 * LENT:
                @pl.when(near)
                def _():
                    drain_recv(hx_recv.at[u // 2], gr.at[pl.ds(2 * u, 2), pl.ds(0, Z - 1)])

                pl.when(jnp.logical_not(near))(own_ring)
            else:
                own_ring()

    def first_rows():
        with scope("wgrad"):
            drain_recv(ay_recv, ar.at[pl.ds(0, (T - 1) * Q)])
            wait_opposite(0, U // 2)
            acc[...] = rows_product(0, n // 2)

    def next_rows():
        with scope("wgrad2"):
            wait_opposite(U // 2, U - 2)
            acc[...] += rows_product(n // 2, n // 2 - 4)

    def rest(k, u):
        pl.when(near & (k == U + 2))(first_rows)
        relays(k)
        pl.when(k == U)(over_tensor)

        @pl.when(late & (k == U + 2))
        def _():
            share_acts()

        return u

    yields = is_odd & (s > 1)

    @pl.when(yields)
    def _():
        with scope("yield"):
            drain_recv(go_recv, gout)

    lax.fori_loop(U, U + 3 * lag, rest, 0)

    @pl.when(helper)
    def _():
        lax.fori_loop(0, LENT + 4, assist, 0)

    @pl.when(first)
    def _():
        def finish(c, u):
            for h in range(H):
                g = ps[c, y, h].astype(F32)
                for d in range(1, T):
                    g = g + pr[1, c, at_y(d), h].astype(F32)
                gout[c, :, h * C : (h + 1) * C] = g.astype(BF16)
            return u

        with scope("first"):
            drain_recv(p_recv.at[n], pr.at[1, :, pl.ds(0, T - 1)])
            lax.fori_loop(0, n, finish, 0)

    @pl.when(not_first & jnp.logical_not(yields))
    def _():
        with scope("backwait"):
            drain_recv(go_recv, gout)

    out_grads[...] = gout[...]

    pl.when(jnp.logical_not(near))(first_rows)
    next_rows()
    with scope("zwait_last"):
        wait_opposite(U - 2, U)
    with scope("wgrad_last"):
        out_wgrad[...] = ((acc[...] + rows_product(n - 4, 4)) * update_factor).astype(BF16)

    drain_recv(kz_recv, pkz.at[pl.ds(0, Z - 1)])
    pkz[z] = pkm[...]
    most = pkz[0]
    for k in range(1, Z):
        most = jnp.maximum(most, pkz[k])
    out_peaks[...] = most

    with scope("close"):
        drain_send(ky_send, pky.at[pl.ds(0, T - 1)])
        drain_send(kz_send, pkz.at[pl.ds(0, Z - 1)])
        drain_send(a_send, ar.at[pl.ds(0, Q), pl.ds(0, Z - 1)])
        drain_send(ay_send, ar.at[pl.ds(0, (T - 1) * Q)])
        @pl.when(near)
        def _():
            drain_send(z_send, gr.at[pl.ds(0, n - 2 * LENT), pl.ds(0, Z - 1)])
            drain_send(h_send, hb.at[:, 0])

        @pl.when(jnp.logical_not(near))
        def _():
            drain_send(z_send, gr.at[:, pl.ds(0, Z - 1)])

        @pl.when(helper)
        def _():
            drain_send(hz_send, hb.at[:, pl.ds(0, Z - 1)])
            drain_send(hx_send, hb.at[:, pl.ds(0, Z - 1)])


        @pl.when(first)
        def _():
            drain_send(fg_send, pr.at[0, :, pl.ds(0, T - 1)])
            drain_send(p_send, pr.at[0, :, pl.ds(0, T - 1)])

        @pl.when(not_first)
        def _():
            drain_send(p_send, pr.at[0])

        @pl.when(not_last)
        def _():
            drain_send(fo_send, pr.at[0])
            drain_send(go_send, gin)


def finish_kernel(a, g, m, peaks, ha, hw, hg, oa, og, om, na, nw, ng, store):
    stores = [pltpu.make_async_copy(v, o, store.at[i]) for i, (v, o) in enumerate(((a, oa), (g, og), (m, om)))]
    for d in stores:
        d.start()
    for i, (old, new) in enumerate(((ha, na), (hw, nw), (hg, ng))):
        new[:, 1:] = old[:, :-1]
        new[:, 0:1] = peaks[i : i + 1, 0:1]
    for d in stores:
        d.wait()


def step(acts_in, weights, cotangent, hist_act, hist_weight, hist_grad):
    S, Z, T = (lax.axis_size(a) for a in ("pipe", "dp", "tensor"))
    micro, rows, width = acts_in.shape
    depth = weights.shape[1]
    R = min(CHUNK, rows)
    n = micro * rows // R
    H = Z // T
    C = depth // Z
    acts = pltpu.with_memory_space_constraint(acts_in.reshape(n, R, width), pltpu.HBM)
    cot = pltpu.with_memory_space_constraint(cotangent.reshape(n, R, width), pltpu.HBM)
    w = weights.reshape(Z, C, width)
    any_ = pl.BlockSpec(memory_space=pl.ANY)
    hbm = pl.BlockSpec(memory_space=pltpu.HBM)
    vmem = pl.BlockSpec(memory_space=pltpu.VMEM)
    dma = pltpu.SemaphoreType.DMA
    b = lambda *shape: pltpu.VMEM(shape, BF16)
    f = lambda *shape: pltpu.VMEM(shape, F32)
    out_acts, out_grads, out_w, peaks = pl.pallas_call(
        functools.partial(kernel, S, Z, T, n, R),
        out_shape=(
            jax.ShapeDtypeStruct((n, R, width), BF16),
            jax.ShapeDtypeStruct((n, R, width), BF16),
            jax.ShapeDtypeStruct((C, width), BF16),
            jax.ShapeDtypeStruct((8, 128), F32),
        ),
        in_specs=[any_] * 6,
        out_specs=(vmem, vmem, vmem, vmem),
        scratch_shapes=[
            b(Z, C, width), b(T, width, width), b(n, Z, R, C), b(n, Z, R, C), b(n, Z, R, C), b(n, Z, R, width),
            b(n, H, R, C), b(n, R, width), b(n, R, width), b(n, R, width),
            b(n, T, H, R, C), b(2, n, T, H, R, C), b(n, R, width), b(2 * LENT, Z, R, width), f(C, width),
            f(H, 1, C), f(1, width), f(1, width),
            f(8, 128), f(T, 8, 128), f(8, 128), f(Z, 8, 128),
            dma((Z,)), dma, dma,
            dma((n, T)), *(dma,) * 7, dma((n + 1,)), dma, dma, dma, dma((n // 2, 6)), dma((n // 2,)),
            dma, dma((LENT,)), dma, dma((LENT, 6)), dma((LENT,)), dma, dma((LENT,)),
            *(dma,) * 4, pltpu.SemaphoreType.REGULAR((2,)), f(3, *hist_act.shape), dma((3,)),
        ],
        compiler_params=pltpu.CompilerParams(
            collective_id=0, has_side_effects=True, vmem_limit_bytes=52000000
        ),
    )(acts, w, cot, *(pltpu.with_memory_space_constraint(h, pltpu.HBM) for h in (hist_act, hist_weight, hist_grad)))

    final = pl.pallas_call(
        finish_kernel,
        out_shape=(
            jax.ShapeDtypeStruct((n, R, width), BF16),
            jax.ShapeDtypeStruct((n, R, width), BF16),
            jax.ShapeDtypeStruct((C, width), BF16),
            *(jax.ShapeDtypeStruct(hist_act.shape, F32) for _ in range(3)),
        ),
        in_specs=[vmem] * 7,
        out_specs=(hbm, hbm, hbm, vmem, vmem, vmem),
        scratch_shapes=[dma((3,))],
        compiler_params=pltpu.CompilerParams(vmem_limit_bytes=8 * 1024 * 1024),
    )(out_acts, out_grads, out_w, peaks, hist_act, hist_weight, hist_grad)
    return (
        final[0].reshape(1, micro, rows, width),
        final[1].reshape(1, micro, rows, width),
        final[2][None],
        *final[3:],
    )


def solution(mesh):
    placed = (
        P(None, "dp", "tensor"),
        P("pipe", None, "tensor"),
        P(None, "dp", "tensor"),
        P("pipe", None),
        P("pipe", None),
        P("pipe", None),
    )
    return jax.shard_map(
        step,
        mesh=mesh,
        in_specs=placed,
        out_specs=(
            P("pipe", None, "dp", "tensor"),
            P("pipe", None, "dp", "tensor"),
            P("pipe", "dp", "tensor"),
            P("pipe", None),
            P("pipe", None),
            P("pipe", None),
        ),
        check_vma=False,
    )
```

```python
import contextlib
import functools

import jax
import jax.numpy as jnp
from jax import lax
from jax.experimental import pallas as pl
from jax.experimental.pallas import tpu as pltpu
from jax.sharding import PartitionSpec as P

MESH = pl.DeviceIdType.MESH
F32 = jnp.float32
BF16 = jnp.bfloat16
CHUNK = 16
AHEAD = 5
WARM = 10
LENT = 2

scope = lambda name: contextlib.nullcontext()


def quantize(values, factor, limit):
    return jnp.clip(values.astype(F32) * factor, -limit, limit).astype(BF16)


def gray(j):
    return j ^ (j >> 1)


def kernel(
    S, Z, T, n, R,
    acts, weights, cot, hist_act, hist_weight, hist_grad,
    out_acts, out_grads, out_wgrad, out_peaks,
    w, wt, xg, xq, ar, gr, outv, gin, gout, gq, ps, pr, cotv, hb, acc, amax, wmax, gmax, pks, pky, pkm, pkz,
    ld_w, ld_x, ld_c,
    f_recv, fg_send, fo_send, a_send, a_recv, ay_send, ay_recv, p_send, p_recv, go_send, go_recv,
    z_send, zr_recv, zo_recv,
    h_send, h_recv, hz_send, hr_recv, ho_recv, hx_send, hx_recv,
    ky_send, ky_recv, kz_send, kz_recv, far, hist, ld_h,
):
    s = lax.axis_index("pipe")
    z = lax.axis_index("dp")
    y = lax.axis_index("tensor")
    H = Z // T
    C = w.shape[1]
    U = n // 2
    Q = n // T
    odd = lax.rem(s, 2)
    even = odd == 0
    is_odd = odd == 1
    first = s == 0
    last = s == S - 1
    not_last = jnp.logical_not(last)
    near = s < 2
    helper = s >= S - 2
    most_lent = first | (s == S - 2)
    loans = jnp.where(most_lent, LENT, LENT - 1)
    buddy = jnp.where(near, s + S - 2, jnp.maximum(s - (S - 2), 0))
    not_first = jnp.logical_not(first)
    up = jnp.minimum(s + 1, S - 1)
    down = jnp.maximum(s - 1, 0)

    def at_y(d):
        return lax.rem(y + d, T)

    def at_z(d):
        return lax.rem(z + d, Z)

    def rcopy(src, dst, send, recv, **device):
        return pltpu.make_async_remote_copy(
            src_ref=src, dst_ref=dst, send_sem=send, recv_sem=recv, device_id=device, device_id_type=MESH
        )

    def drain_send(sem, ref):
        rcopy(ref, ref, sem, sem, tensor=at_y(1)).wait_send()

    def drain_recv(sem, ref):
        rcopy(ref, ref, sem, sem, tensor=at_y(1)).wait_recv()

    barrier = pltpu.get_barrier_semaphore()
    for d in range(1, T):
        pl.semaphore_signal(barrier, inc=1, device_id={"tensor": at_y(d)}, device_id_type=MESH)
    for d in (1, Z - 1):
        pl.semaphore_signal(barrier, inc=1, device_id={"dp": at_z(d)}, device_id_type=MESH)
    for d in range(T):
        @pl.when(not_last)
        def _():
            pl.semaphore_signal(barrier, inc=1, device_id={"pipe": up, "tensor": at_y(d)}, device_id_type=MESH)

        @pl.when(not_first)
        def _():
            pl.semaphore_signal(barrier, inc=1, device_id={"pipe": down, "tensor": at_y(d)}, device_id_type=MESH)

    @pl.when(near | helper)
    def _():
        pl.semaphore_signal(barrier, inc=1, device_id={"pipe": buddy}, device_id_type=MESH)

    own = pl.ds(y * H, H)

    def load_w(r):
        return pltpu.make_async_copy(weights.at[r], w.at[r], ld_w.at[r])

    def load_x(h):
        return pltpu.make_async_copy(acts.at[:, :, pl.ds(h * C, C)], xg.at[:, y * H + h], ld_x)

    load_c = pltpu.make_async_copy(cot, cotv, ld_c)
    load_h = [
        pltpu.make_async_copy(old, hist.at[i], ld_h.at[i])
        for i, old in enumerate((hist_act, hist_weight, hist_grad))
    ]
    for load in load_h:
        load.start()

    @pl.when(first)
    def _():
        for h in range(H):
            load_x(h).start()

    lax.fori_loop(0, Z, lambda r, u: (load_w(r).start(), u)[1], 0)

    @pl.when(last)
    def _():
        load_c.start()

    for load in load_h:
        load.wait()
    ha = jnp.max(hist[0], axis=1, keepdims=True)
    hw = jnp.max(hist[1], axis=1, keepdims=True)
    hg = jnp.max(hist[2], axis=1, keepdims=True)
    act_factor = 448.0 / ha
    weight_factor = 448.0 / hw
    grad_factor = 57344.0 / hg
    forward_factor = 1.0 / (act_factor * weight_factor)
    backward_factor = 1.0 / (grad_factor * weight_factor)
    update_factor = 1.0 / (act_factor * grad_factor)

    amax[...] = jnp.zeros_like(amax)
    wmax[...] = jnp.zeros_like(wmax)
    gmax[...] = jnp.zeros_like(gmax)

    @pl.when(first)
    def _():
        pltpu.make_async_copy(xg.at[:, own], xg.at[:, own], ld_x).wait()


    def gather_copy(c, d):
        return rcopy(xg.at[c, own], xg.at[c, own], fg_send, f_recv.at[c, y], tensor=at_y(d))

    def out_copy(c, d):
        return rcopy(outv.at[c], xg.at[c, own], fo_send, f_recv.at[c, y], pipe=up, tensor=at_y(d))

    def wait_block(c, yb):
        drain_recv(f_recv.at[c, yb], xg.at[c, pl.ds(yb * H, H)])

    def act_copy(c, m, d):
        r = at_z(d)
        span = pl.ds(c, m)
        return rcopy(xq.at[span, r], ar.at[span, z], a_send, a_recv, dp=r)

    def share_copy(d, j):
        span = pl.ds(2 * (y + T * j), 2)
        return rcopy(ar.at[span], ar.at[span], ay_send, ay_recv, tensor=at_y(d))

    def share_acts():
        with scope("share"):
            drain_recv(a_recv, ar.at[pl.ds(0, Q), pl.ds(0, Z - 1)])
            for j in range(U // T):
                for d in (2, 1, 3):
                    share_copy(d, j).start()

    def quant_w(r, u):
        load_w(r).wait()
        raw = w[r].astype(F32)
        wmax[...] = jnp.maximum(wmax[...], jnp.max(jnp.abs(raw), axis=0, keepdims=True))
        w[r] = jnp.clip(raw * weight_factor, -448.0, 448.0).astype(BF16)
        return u

    def turn_w(k, u):
        for h in range(H):
            wt[k, :, h * C : (h + 1) * C] = w[k * H + h].T
        return u

    with scope("qw"):
        lax.fori_loop(0, Z, quant_w, 0)

    with scope("barrier"):
        pairs = not_first.astype(jnp.int32) + not_last.astype(jnp.int32)
        pl.semaphore_wait(barrier, (T - 1) + 2 + T * pairs + (near | helper).astype(jnp.int32))

    def start_gather(c):
        for d in (2, 1, 3):
            gather_copy(c, d).start()

    @pl.when(first)
    def _():
        for c in range(AHEAD):
            start_gather(c)

    def far_signal(level):
        for to in (level + 1, Z - 1 - level):
            pl.semaphore_signal(far.at[level], inc=1, device_id={"dp": at_z(to)}, device_id_type=MESH)

    far_signal(0)

    late = s >= S // 2
    early = jnp.logical_not(late)

    @pl.when(late)
    def _():
        with scope("turn"):
            lax.fori_loop(0, T, turn_w, 0)

    with scope("far0"):
        pl.semaphore_wait(far.at[0], 2)
        far_signal(1)

    def forward(c, m):
        span = pl.ds(c, m)
        total = jnp.zeros((m * R, H * C), F32)
        for j in range(T):
            yb = at_y((2 * (1 - odd), 1, 3, 2 * odd)[j])

            def take():
                with scope(f"fwait{j}"):
                    for i in range(m):
                        wait_block(c + i, yb)

            if m > 1 or j < T - 1:
                take()
            else:
                pl.when(not_first)(take)

            for h in range(H):
                r = yb * H + h
                q = quantize(xg[span, r].reshape(m * R, C), act_factor, 448.0)
                xq[span, r] = q.reshape(m, R, C)
                total = total + jnp.dot(q, w[r], preferred_element_type=F32)
        for h in range(H):
            x = xg[span, y * H + h].reshape(m * R, C).astype(F32)
            o = x + total[:, h * C : (h + 1) * C] * forward_factor
            outv[span, h] = o.astype(BF16).reshape(m, R, C)

        def send():
            for i in range(m):
                for d in (2, 1, 3, 0):
                    out_copy(c + i, d).start()

        if m == 1:
            send()
        else:
            pl.when(not_last)(send)

        with scope("fz"):
            if m == 1:
                @pl.when(first & (c + AHEAD < n))
                def _():
                    start_gather(c + AHEAD)

            @pl.when(c == 0)
            def _():
                pl.semaphore_wait(far.at[1], 2)

            @pl.when(lax.rem(c // 2, T) == y)
            def _():
                for d in (4, 3, 5, 2, 6, 1, 7):
                    act_copy(c, m, d).start()
                ar[span, z] = xq[span, z]

            for h in range(H):
                out_acts[span, :, h * C : (h + 1) * C] = outv[span, h]
                x = xg[span, y * H + h].reshape(m * R, C).astype(F32)
                amax[h] = jnp.maximum(amax[h], jnp.max(jnp.abs(x), axis=0, keepdims=True))

    side = first.astype(jnp.int32)

    def part_copy(c, d):
        yb = at_y(d)
        recv = p_recv.at[jnp.where(first, n, c)]
        return rcopy(ps.at[c, yb], pr.at[side, c, y], p_send, recv, pipe=down, tensor=yb)

    def back_copy(c):
        return rcopy(gin.at[c], gout.at[c], go_send, go_recv, pipe=up)

    def ring_copy(u, back):
        span = pl.ds(2 * u, 2)
        return rcopy(gq.at[span], gr.at[span, z], z_send, zr_recv.at[u, 3 * back], dp=at_z(Z - 1 if back else 1))

    def relay_copy(u, level, back):
        k = at_z(level if back else Z - level)
        span = pl.ds(2 * u, 2)
        if level < 3:
            ref = gr.at[span, k]
            recv = zr_recv.at[u, 3 * back + level]
        else:
            half = H * C // 2
            ref = gr.at[span, k, :, pl.ds(half * back, half)]
            recv = zo_recv.at[u]
        return rcopy(ref, ref, z_send, recv, dp=at_z(Z - 1 if back else 1))

    lag = jnp.where(s < 2, 1, 3)

    def skip_copy(u, back):
        span = pl.ds(2 * u, 2)
        return rcopy(gq.at[span], gr.at[span, z], z_send, zr_recv.at[u, 3 * back + 1], dp=at_z(Z - 2 if back else 2))

    def over_copy(u, back):
        half = H * C // 2
        ref = gr.at[pl.ds(2 * u, 2), at_z(2 if back else Z - 2), :, pl.ds(half * back, half)]
        return rcopy(ref, ref, z_send, zo_recv.at[u], dp=at_z(Z - 2 if back else 2))

    def lent(u):
        return near & (lax.rem(u, 2) == 1) & (u < 2 * loans)

    def lend_copy(u):
        i = u // 2
        return rcopy(gq.at[pl.ds(2 * u, 2)], hb.at[pl.ds(2 * i, 2), z], h_send, h_recv.at[i], pipe=buddy)

    def help_copy(i, level, back):
        span = pl.ds(2 * i, 2)
        k = at_z(level if back else Z - level) if level else z
        if level < 3:
            ref, recv = hb.at[span, k], hr_recv.at[i, 3 * back + level]
        else:
            half = H * C // 2
            ref, recv = hb.at[span, k, :, pl.ds(half * back, half)], ho_recv.at[i]
        return rcopy(ref, ref, hz_send, recv, dp=at_z(Z - 1 if back else 1))

    def return_copy(i, k):
        return rcopy(hb.at[pl.ds(2 * i, 2), k], gr.at[pl.ds(4 * i + 2, 2), k], hx_send, hx_recv.at[i], pipe=buddy)

    def assist(t, v):
        for level in range(5):
            i = t - level

            @pl.when((i >= 0) & (i < loans))
            def _():
                span = pl.ds(2 * i, 2)
                with scope(f"assist{level}"):
                    if level == 0:
                        drain_recv(h_recv.at[i], hb.at[span, z])
                        help_copy(i, 0, 0).start()
                        help_copy(i, 0, 1).start()
                    elif level < 4:
                        for back in (0, 1):
                            k = at_z(level if back else Z - level)
                            drain_recv(hr_recv.at[i, 3 * back + level - 1], hb.at[span, k])
                            help_copy(i, level, back).start()
                            return_copy(i, k).start()
                    else:
                        drain_recv(ho_recv.at[i], hb.at[span, at_z(4)])
                        return_copy(i, at_z(4)).start()

        return v

    def short(u):
        return first & (u == U - 1)

    def relays(t, levels=(1, 2, 3)):
        for level in levels:
            u = t - lag * level

            @pl.when((u >= 0) & (u < U) & jnp.logical_not(lent(u)))
            def _():
                with scope(f"relay{level}"):
                    for back in (0, 1):
                        k = at_z(level if back else Z - level)
                        drain_recv(zr_recv.at[u, 3 * back + level - 1], gr.at[pl.ds(2 * u, 2), k])
                        if level == 2:
                            relay_copy(u, level, back).start()

                            @pl.when(short(u))
                            def _():
                                over_copy(u, back).start()
                        else:
                            @pl.when(jnp.logical_not(short(u)))
                            def _():
                                relay_copy(u, level, back).start()

    @pl.when(last)
    def _():
        load_c.wait()

    def backward(c, m):
        span = pl.ds(c, m)
        def begin():
            for h in range(H):
                part = cotv[span, :, h * C : (h + 1) * C].astype(F32) * outv[span, h].astype(F32)
                gin[span, :, h * C : (h + 1) * C] = part.astype(BF16)

        def arrive():
            with scope("bwait"):
                for i in range(m):
                    drain_recv(p_recv.at[c + i], pr.at[0, c + i])
            for h in range(H):
                g = pr[0, span, 0, h].astype(F32)
                for k in range(1, T):
                    g = g + pr[0, span, k, h].astype(F32)
                gin[span, :, h * C : (h + 1) * C] = g.astype(BF16)

        if m > 1:
            pl.when(last)(begin)
            pl.when(not_last)(arrive)
        else:
            arrive()
        g = gin[span].reshape(m * R, H * C)
        q = quantize(g, grad_factor, 57344.0)
        gq[span] = q.reshape(m, R, H * C)
        for d in (2, 1, 3, 0):
            yb = at_y(d)
            part = jnp.dot(q, wt[yb], preferred_element_type=F32) * backward_factor
            if d == 0:
                part = part + g.astype(F32)
            for h in range(H):
                ps[span, yb, h] = part[:, h * C : (h + 1) * C].astype(BF16).reshape(m, R, C)
            if d:
                for i in range(m):
                    part_copy(c + i, d).start()

        def to_own():
            for i in range(m):
                part_copy(c + i, 0).start()

        if m > 1:
            to_own()

            @pl.when(not_last)
            def _():
                for i in range(m):
                    back_copy(c + i).start()
        else:
            pl.when(not_first)(to_own)
            back_copy(c).start()
        with scope("bz"):
            gmax[...] = jnp.maximum(gmax[...], jnp.max(jnp.abs(g.astype(F32)), axis=0, keepdims=True))
            gr[span, z] = q.reshape(m, R, H * C)

    prior = s == S - 2
    inner = not_last & jnp.logical_not(prior)
    warm = jnp.where(last, 0, jnp.where(prior, WARM, n))

    def slot(k, u):
        ahead = k < warm
        pairs = jnp.logical_not(ahead) & jnp.logical_not(inner)
        late_k = k - warm
        mixed = jnp.logical_not(ahead) & (late_k < n - warm)
        turn = lax.rem(late_k, 2)
        fwd_pair = pairs & mixed & jnp.where(last, turn == 0, turn == 1)
        bwd_pair = pairs & jnp.logical_not(fwd_pair)
        bwd_one = jnp.logical_not(ahead) & inner
        f_at = warm + 2 * (late_k // 2)
        b_at = jnp.where(mixed, 2 * (late_k // 2), n - warm + 2 * (late_k - (n - warm)))

        @pl.when(ahead)
        def _():
            forward(k, 1)

        @pl.when(fwd_pair)
        def _():
            forward(f_at, 2)

        @pl.when(bwd_pair)
        def _():
            backward(b_at, 2)

        @pl.when(bwd_one)
        def _():
            backward(late_k, 1)

        unit = jnp.where(inner, late_k, b_at) // 2

        @pl.when(bwd_pair | (bwd_one & (lax.rem(late_k, 2) == 1)))
        def _():
            @pl.when(short(unit))
            def _():
                skip_copy(unit, 0).start()
                skip_copy(unit, 1).start()

            @pl.when(lent(unit))
            def _():
                lend_copy(unit).start()

            @pl.when(jnp.logical_not(lent(unit)))
            def _():
                ring_copy(unit, 0).start()
                ring_copy(unit, 1).start()

            relays(unit)

        @pl.when(early & (k == n - 1))
        def _():
            with scope("turn"):
                lax.fori_loop(0, T, turn_w, 0)
            share_acts()

        return u

    lax.fori_loop(0, jnp.where(inner, 2 * n, jnp.where(last, n, n + WARM // 2)), slot, 0)

    lanes = pks.shape[-1]
    peak_a = jnp.max(jnp.maximum(amax[0], amax[H - 1]), axis=1, keepdims=True)
    peak_w = jnp.max(wmax[...], axis=1, keepdims=True)
    peak_g = jnp.max(gmax[...], axis=1, keepdims=True)
    row = lax.broadcasted_iota(jnp.int32, (8, lanes), 0)
    tile = jnp.where(row == 0, peak_a, jnp.where(row == 1, peak_w, peak_g))
    pks[...] = tile

    def ky_copy(d):
        return rcopy(pks, pky.at[y], ky_send, ky_recv, tensor=at_y(d))

    def kz_copy(d):
        return rcopy(pkm, pkz.at[z], kz_send, kz_recv, dp=at_z(d))

    for d in range(1, T):
        ky_copy(d).start()

    def over_tensor():
        with scope("kwait"):
            drain_recv(ky_recv, pky.at[pl.ds(0, T - 1)])
        pky[y] = pks[...]
        most = pky[0]
        for k in range(1, T):
            most = jnp.maximum(most, pky[k])
        pkm[...] = most
        for d in range(1, Z):
            kz_copy(d).start()

    def rows_product(lo, count):
        left = ar[lo : lo + count].reshape(count * Z * R, C)
        right = gr[lo : lo + count].reshape(count * Z * R, H * C)
        return lax.dot_general(left, right, (((0,), (0,)), ((), ())), preferred_element_type=F32)

    def wait_opposite(lo, hi):
        for u in range(lo, hi):
            def own_ring():
                drain_recv(zo_recv.at[u], gr.at[pl.ds(2 * u, 2), 0])

            if u % 2 == 1 and u < 2 * LENT:
                by_helper = near if u < 2 * LENT - 2 else first

                @pl.when(by_helper)
                def _():
                    drain_recv(hx_recv.at[u // 2], gr.at[pl.ds(2 * u, 2), pl.ds(0, Z - 1)])

                pl.when(jnp.logical_not(by_helper))(own_ring)
            else:
                own_ring()

    def first_rows():
        with scope("wgrad"):
            drain_recv(ay_recv, ar.at[pl.ds(0, (T - 1) * Q)])
            wait_opposite(0, U // 2)
            acc[...] = rows_product(0, n // 2)

    def next_rows():
        with scope("wgrad2"):
            wait_opposite(U // 2, U - 2)
            acc[...] += rows_product(n // 2, n // 2 - 4)

    def own_grads():
        def finish(c, u):
            for h in range(H):
                g = ps[c, y, h].astype(F32)
                for d in range(1, T):
                    g = g + pr[1, c, at_y(d), h].astype(F32)
                gout[c, :, h * C : (h + 1) * C] = g.astype(BF16)
            return u

        with scope("first"):
            drain_recv(p_recv.at[n], pr.at[1, :, pl.ds(0, T - 1)])
            lax.fori_loop(0, n, finish, 0)

    def rest(k, u):
        @pl.when(first & (k == U + 2))
        def _():
            own_grads()
            next_rows()

        relays(k, (1, 2))
        pl.when(first & (k == U + 1))(first_rows)
        relays(k, (3,))
        pl.when(k == U)(over_tensor)

        @pl.when(late & (k == U + 2))
        def _():
            share_acts()

        return u

    yields = is_odd & (s > 1)

    @pl.when(yields)
    def _():
        with scope("yield"):
            drain_recv(go_recv, gout)

    lax.fori_loop(U, U + 3 * lag, rest, 0)

    @pl.when(helper)
    def _():
        lax.fori_loop(0, loans + 4, assist, 0)

    @pl.when(not_first & jnp.logical_not(yields))
    def _():
        with scope("backwait"):
            drain_recv(go_recv, gout)

    out_grads[...] = gout[...]

    @pl.when(not_first)
    def _():
        first_rows()
        next_rows()

    with scope("zwait_last"):
        wait_opposite(U - 2, U)
    with scope("wgrad_last"):
        out_wgrad[...] = ((acc[...] + rows_product(n - 4, 4)) * update_factor).astype(BF16)

    drain_recv(kz_recv, pkz.at[pl.ds(0, Z - 1)])
    pkz[z] = pkm[...]
    most = pkz[0]
    for k in range(1, Z):
        most = jnp.maximum(most, pkz[k])
    out_peaks[...] = most

    with scope("close"):
        drain_send(ky_send, pky.at[pl.ds(0, T - 1)])
        drain_send(kz_send, pkz.at[pl.ds(0, Z - 1)])
        drain_send(a_send, ar.at[pl.ds(0, Q), pl.ds(0, Z - 1)])
        drain_send(ay_send, ar.at[pl.ds(0, (T - 1) * Q)])
        for who, count in ((most_lent, LENT), (jnp.logical_not(most_lent), LENT - 1)):
            @pl.when(near & who)
            def _():
                drain_send(z_send, gr.at[pl.ds(0, n - 2 * count), pl.ds(0, Z - 1)])
                drain_send(h_send, hb.at[pl.ds(0, 2 * count), 0])

            @pl.when(helper & who)
            def _():
                drain_send(hz_send, hb.at[pl.ds(0, 2 * count), pl.ds(0, Z - 1)])
                drain_send(hx_send, hb.at[pl.ds(0, 2 * count), pl.ds(0, Z - 1)])

        @pl.when(jnp.logical_not(near))
        def _():
            drain_send(z_send, gr.at[:, pl.ds(0, Z - 1)])


        @pl.when(first)
        def _():
            drain_send(fg_send, pr.at[0, :, pl.ds(0, T - 1)])
            drain_send(p_send, pr.at[0, :, pl.ds(0, T - 1)])

        @pl.when(not_first)
        def _():
            drain_send(p_send, pr.at[0])

        @pl.when(not_last)
        def _():
            drain_send(fo_send, pr.at[0])
            drain_send(go_send, gin)


def finish_kernel(a, g, m, peaks, ha, hw, hg, oa, og, om, na, nw, ng, store):
    stores = [pltpu.make_async_copy(v, o, store.at[i]) for i, (v, o) in enumerate(((a, oa), (g, og), (m, om)))]
    for d in stores:
        d.start()
    for i, (old, new) in enumerate(((ha, na), (hw, nw), (hg, ng))):
        new[:, 1:] = old[:, :-1]
        new[:, 0:1] = peaks[i : i + 1, 0:1]
    for d in stores:
        d.wait()


def step(acts_in, weights, cotangent, hist_act, hist_weight, hist_grad):
    S, Z, T = (lax.axis_size(a) for a in ("pipe", "dp", "tensor"))
    micro, rows, width = acts_in.shape
    depth = weights.shape[1]
    R = min(CHUNK, rows)
    n = micro * rows // R
    H = Z // T
    C = depth // Z
    acts = pltpu.with_memory_space_constraint(acts_in.reshape(n, R, width), pltpu.HBM)
    cot = pltpu.with_memory_space_constraint(cotangent.reshape(n, R, width), pltpu.HBM)
    w = weights.reshape(Z, C, width)
    any_ = pl.BlockSpec(memory_space=pl.ANY)
    hbm = pl.BlockSpec(memory_space=pltpu.HBM)
    vmem = pl.BlockSpec(memory_space=pltpu.VMEM)
    dma = pltpu.SemaphoreType.DMA
    b = lambda *shape: pltpu.VMEM(shape, BF16)
    f = lambda *shape: pltpu.VMEM(shape, F32)
    out_acts, out_grads, out_w, peaks = pl.pallas_call(
        functools.partial(kernel, S, Z, T, n, R),
        out_shape=(
            jax.ShapeDtypeStruct((n, R, width), BF16),
            jax.ShapeDtypeStruct((n, R, width), BF16),
            jax.ShapeDtypeStruct((C, width), BF16),
            jax.ShapeDtypeStruct((8, 128), F32),
        ),
        in_specs=[any_] * 6,
        out_specs=(vmem, vmem, vmem, vmem),
        scratch_shapes=[
            b(Z, C, width), b(T, width, width), b(n, Z, R, C), b(n, Z, R, C), b(n, Z, R, C), b(n, Z, R, width),
            b(n, H, R, C), b(n, R, width), b(n, R, width), b(n, R, width),
            b(n, T, H, R, C), b(2, n, T, H, R, C), b(n, R, width), b(2 * LENT, Z, R, width), f(C, width),
            f(H, 1, C), f(1, width), f(1, width),
            f(8, 128), f(T, 8, 128), f(8, 128), f(Z, 8, 128),
            dma((Z,)), dma, dma,
            dma((n, T)), *(dma,) * 7, dma((n + 1,)), dma, dma, dma, dma((n // 2, 6)), dma((n // 2,)),
            dma, dma((LENT,)), dma, dma((LENT, 6)), dma((LENT,)), dma, dma((LENT,)),
            *(dma,) * 4, pltpu.SemaphoreType.REGULAR((2,)), f(3, *hist_act.shape), dma((3,)),
        ],
        compiler_params=pltpu.CompilerParams(
            collective_id=0, has_side_effects=True, vmem_limit_bytes=52000000
        ),
    )(acts, w, cot, *(pltpu.with_memory_space_constraint(h, pltpu.HBM) for h in (hist_act, hist_weight, hist_grad)))

    final = pl.pallas_call(
        finish_kernel,
        out_shape=(
            jax.ShapeDtypeStruct((n, R, width), BF16),
            jax.ShapeDtypeStruct((n, R, width), BF16),
            jax.ShapeDtypeStruct((C, width), BF16),
            *(jax.ShapeDtypeStruct(hist_act.shape, F32) for _ in range(3)),
        ),
        in_specs=[vmem] * 7,
        out_specs=(hbm, hbm, hbm, vmem, vmem, vmem),
        scratch_shapes=[dma((3,))],
        compiler_params=pltpu.CompilerParams(vmem_limit_bytes=8 * 1024 * 1024),
    )(out_acts, out_grads, out_w, peaks, hist_act, hist_weight, hist_grad)
    return (
        final[0].reshape(1, micro, rows, width),
        final[1].reshape(1, micro, rows, width),
        final[2][None],
        *final[3:],
    )


def solution(mesh):
    placed = (
        P(None, "dp", "tensor"),
        P("pipe", None, "tensor"),
        P(None, "dp", "tensor"),
        P("pipe", None),
        P("pipe", None),
        P("pipe", None),
    )
    return jax.shard_map(
        step,
        mesh=mesh,
        in_specs=placed,
        out_specs=(
            P("pipe", None, "dp", "tensor"),
            P("pipe", None, "dp", "tensor"),
            P("pipe", "dp", "tensor"),
            P("pipe", None),
            P("pipe", None),
            P("pipe", None),
        ),
        check_vma=False,
    )
```
